8 devices in a mesh: fsdp: 8 (over z, y, x, core).
Axes of the slice: x: 2, y: 2, z: 1, core: 2. Of those that a mesh axis runs over, the one named last changes fastest.
Arguments:
- tokens: int32 [64, 256], P('fsdp')
- positions: int32 [64, 256], P('fsdp')
- embed_table: bfloat16 [152064, 1024], P('fsdp')
- attn_norm: bfloat16 [1024], P('fsdp')
- w_query: bfloat16 [1024, 2048], P('fsdp')
- w_key: bfloat16 [1024, 1024], P('fsdp')
- w_value: bfloat16 [1024, 1024], P('fsdp')
- q_norm: bfloat16 [128], replicated
- k_norm: bfloat16 [128], replicated
- w_out: bfloat16 [2048, 1024], P('fsdp')
- mlp_norm: bfloat16 [1024], P('fsdp')
- w_gate: bfloat16 [1024, 3072], P('fsdp')
- w_up: bfloat16 [1024, 3072], P('fsdp')
- w_down: bfloat16 [3072, 1024], P('fsdp')
- dy_out: bfloat16 [64, 256, 1024], P('fsdp')
Outputs:
- output 1: bfloat16 [64, 256, 1024], P('fsdp')
- output 2: float32 [152064, 1024], P('fsdp')
- output 3: float32 [1024], P('fsdp')
- output 4: float32 [1024, 2048], P('fsdp')
- output 5: float32 [1024, 1024], P('fsdp')
- output 6: float32 [1024, 1024], P('fsdp')
- output 7: float32 [128], replicated
- output 8: float32 [128], replicated
- output 9: float32 [2048, 1024], P('fsdp')
- output 10: float32 [1024], P('fsdp')
- output 11: float32 [1024, 3072], P('fsdp')
- output 12: float32 [1024, 3072], P('fsdp')
- output 13: float32 [3072, 1024], P('fsdp')
All inputs are finite; a program needn't handle non-finite values.
Results may differ from the reference program's by a relative error of at most 0.0159861.
Values are sent between devices in bfloat16 or wider.
A program may use at most 1 GiB of HBM per device.

```python
import math
import jax
import jax.numpy as jnp
from jax import lax

D = 1024
HEADS = 16
KV_HEADS = 8
HEAD = 128
FF = 3072
VOCAB = 151936
VOCAB_P = 152064
GROUP = 8
BATCH_DEV = 8
SEQ = 256

BATCH = GROUP * BATCH_DEV
Q_PER_KV = HEADS // KV_HEADS
ROWS_SHARD = VOCAB_P // GROUP
DOC_SPAN = max(SEQ // 4, 2)
NORM_EPS = 1e-6
ROPE_THETA = 1.0e6


def draw_tokens(rng_key):
    key_list = jax.random.split(rng_key, 4)
    id_top = jax.random.randint(key_list[0], (BATCH, SEQ), 1, VOCAB + 1)
    id_mid = jax.random.randint(key_list[1], (BATCH, SEQ), 0, id_top)
    token_ids = jax.random.randint(key_list[2], (BATCH, SEQ), 0, id_mid + 1)
    shard_lo = (jnp.arange(BATCH) % GROUP) * ROWS_SHARD
    shard_hi = jnp.minimum(shard_lo + ROWS_SHARD, VOCAB)
    cover_ids = jax.random.randint(key_list[3], (BATCH,), shard_lo, shard_hi)
    token_ids = token_ids.at[:, 0].set(cover_ids)
    return token_ids.at[BATCH - 1, SEQ - 1].set(VOCAB - 1).astype(jnp.int32)


def draw_positions(rng_key):
    seq_idx = jnp.arange(SEQ, dtype=jnp.int32)[None, :]
    starts = (jax.random.randint(rng_key, (BATCH, SEQ), 0, DOC_SPAN) == 0) | (seq_idx == 0)
    last_start = lax.cummax(jnp.where(starts, seq_idx, 0), axis=1)
    return (seq_idx - last_start).astype(jnp.int32)


def setup_inputs(seed: int = 0) -> dict:
    key_list = jax.random.split(jax.random.key(seed), 16)

    def weight(key_idx, arr_shape, fan_in):
        return (jax.random.normal(key_list[key_idx], arr_shape, jnp.float32) * fan_in ** -0.5).astype(jnp.bfloat16)

    def gain_vec(key_idx, vec_len):
        return (1.0 + 0.25 * jax.random.normal(key_list[key_idx], (vec_len,), jnp.float32)).astype(jnp.bfloat16)

    table_f = jax.random.normal(key_list[2], (VOCAB_P, D), jnp.float32)
    table_f = jnp.where(jnp.arange(VOCAB_P)[:, None] < VOCAB, table_f, 0.0)
    return {
        'tokens': draw_tokens(key_list[0]),
        'positions': draw_positions(key_list[1]),
        'embed_table': table_f.astype(jnp.bfloat16),
        'attn_norm': gain_vec(3, D),
        'w_query': weight(4, (D, HEADS * HEAD), D),
        'w_key': weight(5, (D, KV_HEADS * HEAD), D),
        'w_value': weight(6, (D, KV_HEADS * HEAD), D),
        'q_norm': gain_vec(7, HEAD),
        'k_norm': gain_vec(8, HEAD),
        'w_out': weight(9, (HEADS * HEAD, D), HEADS * HEAD),
        'mlp_norm': gain_vec(10, D),
        'w_gate': weight(11, (D, FF), D),
        'w_up': weight(12, (D, FF), D),
        'w_down': weight(13, (FF, D), FF),
        'dy_out': jax.random.normal(key_list[14], (BATCH, SEQ, D), jnp.float32).astype(jnp.bfloat16),
    }


def to_bf16(values):
    return values + lax.stop_gradient(values.astype(jnp.bfloat16).astype(jnp.float32) - values)


def rms_scale(values, norm_gain):
    inv_rms = lax.rsqrt(jnp.mean(values * values, axis=-1, keepdims=True) + NORM_EPS)
    return values * inv_rms * norm_gain


def rope_tables(positions):
    half_dim = HEAD // 2
    inv_freq = jnp.exp(jnp.arange(half_dim, dtype=jnp.float32) * (-2.0 * math.log(ROPE_THETA) / HEAD))
    angles = positions.astype(jnp.float32)[:, :, None] * inv_freq
    return jnp.cos(angles), jnp.sin(angles)


def rotate(values, cos_t, sin_t):
    half_dim = values.shape[-1] // 2
    lead_half = values[..., :half_dim]
    tail_half = values[..., half_dim:]
    return jnp.concatenate([lead_half * cos_t - tail_half * sin_t, tail_half * cos_t + lead_half * sin_t], axis=-1)


def seq_attend(operands):
    q_seq, k_seq, v_seq = operands
    scores = jnp.einsum('qgrh,kgh->grqk', q_seq, k_seq) * (HEAD ** -0.5)
    causal = jnp.arange(SEQ)[:, None] >= jnp.arange(SEQ)[None, :]
    scores = jnp.where(causal, scores, -1e30)
    attn_probs = to_bf16(jax.nn.softmax(scores, axis=-1))
    return to_bf16(jnp.einsum('grqk,kgh->qgrh', attn_probs, v_seq))


def reference(tokens, positions, embed_table, attn_norm, w_query, w_key, w_value, q_norm, k_norm, w_out, mlp_norm, w_gate, w_up, w_down, dy_out):
    cos_t, sin_t = rope_tables(positions)
    cos_q = cos_t[:, :, None, None, :]
    sin_q = sin_t[:, :, None, None, :]
    cos_k = cos_t[:, :, None, :]
    sin_k = sin_t[:, :, None, :]

    def layer_fwd(x_emb, g_attn, wt_query, wt_key, wt_value, g_query, g_key, wt_out, g_mlp, wt_gate, wt_up, wt_down):
        normed = to_bf16(rms_scale(x_emb, g_attn)).reshape(BATCH * SEQ, D)
        q_proj = to_bf16(jnp.dot(normed, wt_query, preferred_element_type=jnp.float32)).reshape(BATCH, SEQ, KV_HEADS, Q_PER_KV, HEAD)
        k_proj = to_bf16(jnp.dot(normed, wt_key, preferred_element_type=jnp.float32)).reshape(BATCH, SEQ, KV_HEADS, HEAD)
        v_proj = to_bf16(jnp.dot(normed, wt_value, preferred_element_type=jnp.float32)).reshape(BATCH, SEQ, KV_HEADS, HEAD)
        q_rot = to_bf16(rotate(rms_scale(q_proj, g_query), cos_q, sin_q))
        k_rot = to_bf16(rotate(rms_scale(k_proj, g_key), cos_k, sin_k))
        attn_heads = lax.map(jax.checkpoint(seq_attend), (q_rot, k_rot, v_proj))
        attn_proj = jnp.dot(attn_heads.reshape(BATCH * SEQ, HEADS * HEAD), wt_out, preferred_element_type=jnp.float32)
        hidden = to_bf16(x_emb + attn_proj.reshape(BATCH, SEQ, D))
        mlp_in = to_bf16(rms_scale(hidden, g_mlp)).reshape(BATCH * SEQ, D)
        gate_pre = jnp.dot(mlp_in, wt_gate, preferred_element_type=jnp.float32)
        up_proj = jnp.dot(mlp_in, wt_up, preferred_element_type=jnp.float32)
        mlp_act = to_bf16(jax.nn.silu(gate_pre) * up_proj)
        mlp_proj = jnp.dot(mlp_act, wt_down, preferred_element_type=jnp.float32)
        return to_bf16(hidden + mlp_proj.reshape(BATCH, SEQ, D))

    x_emb = jnp.take(embed_table, tokens, axis=0).astype(jnp.float32)
    params = [weight_arr.astype(jnp.float32) for weight_arr in (attn_norm, w_query, w_key, w_value, q_norm, k_norm, w_out, mlp_norm, w_gate, w_up, w_down)]
    layer_out, pullback = jax.vjp(layer_fwd, x_emb, *params)
    grad_list = pullback(dy_out.astype(jnp.float32))
    d_table = jax.ops.segment_sum(grad_list[0].reshape(BATCH * SEQ, D), tokens.reshape(BATCH * SEQ), num_segments=VOCAB_P)
    return (layer_out.astype(jnp.bfloat16), d_table, grad_list[1], grad_list[2], grad_list[3], grad_list[4], grad_list[5], grad_list[6], grad_list[7], grad_list[8], grad_list[9], grad_list[10], grad_list[11])
```

```python
import functools
import math
import jax
import jax.numpy as jnp
from jax import lax
from jax.experimental import pallas as pl
from jax.experimental.pallas import tpu as pltpu
from jax.sharding import PartitionSpec as P

NORM_EPS = 1e-6
ROPE_THETA = 1.0e6
AXIS_NAME = 'fsdp'
F32 = jnp.float32
BF16 = jnp.bfloat16
LANES = 128
SUBL = 8
VMEM_LIMIT = 60 * 1024 * 1024


def dot_nt(a, b):
    return lax.dot_general(a, b, (((1,), (1,)), ((), ())), preferred_element_type=F32)


def dot_tn(a, b):
    return lax.dot_general(a, b, (((0,), (0,)), ((), ())), preferred_element_type=F32)


def dot_nn(a, b):
    return jnp.dot(a, b, preferred_element_type=F32)


def block_of(total, limit, step):
    best = step
    for size in range(step, limit + 1, step):
        if total % size == 0:
            best = size
    return best


def gather_body(n_tab, n_lead, tab_rows, tok_rows, idx_ref, tab_ref, lead_ref, tail_ref, store, stage):
    step = pl.program_id(0)

    @pl.when(step == 0)
    def _():
        store[n_tab * tab_rows] = jnp.zeros((SUBL, LANES), BF16)

    @pl.when(step < n_tab)
    def _():
        for lane in range(SUBL):
            stage[pl.ds(lane, tab_rows, stride=SUBL), :] = tab_ref[:, lane * LANES:(lane + 1) * LANES].astype(F32)
        rows = stage[...].reshape(tab_rows, SUBL, LANES)
        store[pl.ds(step * tab_rows, tab_rows)] = rows.astype(BF16)

    def copy_rows(out_ref):
        base = (step - n_tab) * tok_rows
        unroll = 16

        def loop(it, carry):
            first = it * unroll
            for u in range(unroll):
                out_ref[first + u] = store[idx_ref[base + first + u]]
            return carry

        lax.fori_loop(0, tok_rows // unroll, loop, 0)

    @pl.when((step >= n_tab) & (step < n_tab + n_lead))
    def _():
        copy_rows(lead_ref)

    @pl.when(step >= n_tab + n_lead)
    def _():
        copy_rows(tail_ref)


def table_gather(table, idx, lead):
    rows, width = table.shape
    total = idx.shape[0]
    tab_rows = block_of(rows, 640, 16)
    n_tab = rows // tab_rows
    tok_rows = 512
    n_lead, n_tail = lead // tok_rows, (total - lead) // tok_rows
    out_block = (tok_rows, SUBL, LANES)
    grid_spec = pltpu.PrefetchScalarGridSpec(
        num_scalar_prefetch=1,
        grid=(n_tab + n_lead + n_tail,),
        in_specs=[pl.BlockSpec((tab_rows, width), lambda s, ids: (jnp.minimum(s, n_tab - 1), 0))],
        out_specs=[pl.BlockSpec(out_block, lambda s, ids: (jnp.clip(s - n_tab, 0, n_lead - 1), 0, 0)),
                   pl.BlockSpec(out_block, lambda s, ids: (jnp.clip(s - n_tab - n_lead, 0, n_tail - 1), 0, 0))],
        scratch_shapes=[pltpu.VMEM((rows + 8, SUBL, LANES), BF16), pltpu.VMEM((tab_rows * SUBL, LANES), F32)],
    )
    return pl.pallas_call(
        functools.partial(gather_body, n_tab, n_lead, tab_rows, tok_rows),
        grid_spec=grid_spec,
        out_shape=[jax.ShapeDtypeStruct((n * tok_rows, SUBL, LANES), BF16) for n in (n_lead, n_tail)],
        compiler_params=pltpu.CompilerParams(dimension_semantics=("arbitrary",), vmem_limit_bytes=VMEM_LIMIT),
        cost_estimate=pl.CostEstimate(flops=70_000_000_000, bytes_accessed=rows * width * 2 + total * width * 2, transcendentals=0),
        name="table_gather",
    )(idx, table)


def scatter_body(group, slots, out_rows, perm_ref, sid_ref, bst_ref, rows_ref, out_ref, acc, ring, sem):
    blk = pl.program_id(0)
    total = bst_ref[pl.num_programs(0)]
    n_groups = (total + group - 1) // group

    def issue(g):
        slot = lax.rem(g, slots)
        for u in range(group):
            pltpu.make_async_copy(rows_ref.at[perm_ref[g * group + u]], ring.at[slot * group + u], sem.at[slot]).start()

    @pl.when(blk == 0)
    def _():
        def first(g, carry):
            issue(g)
            return carry

        lax.fori_loop(0, jnp.minimum(n_groups, slots), first, 0)

    acc[...] = jnp.zeros(acc.shape, F32)
    low = bst_ref[blk]
    high = bst_ref[blk + 1]
    g_first = low // group
    g_last = jnp.where(high > low, (high + group - 1) // group, g_first)
    base = blk * out_rows

    def per_group(g, carry):
        start = g * group
        slot = lax.rem(g, slots)

        @pl.when(start >= low)
        def _():
            pltpu.make_async_copy(rows_ref.at[pl.ds(0, group)], ring.at[pl.ds(slot * group, group)], sem.at[slot]).wait()

        prev, prev_id = carry
        for u in range(group):
            row_id = sid_ref[start + u]
            local = row_id - base
            inside = (local >= 0) & (local < out_rows)
            value = ring[slot * group + u]
            value = jnp.where(row_id == prev_id, prev + value, value)
            acc[pl.ds(pl.multiple_of(jnp.where(inside, local, out_rows) * SUBL, SUBL), SUBL), :] = value
            prev, prev_id = value, row_id

        @pl.when((high >= start + group) & (g + slots < n_groups))
        def _():
            issue(g + slots)

        return prev, prev_id

    lax.fori_loop(g_first, g_last, per_group, (jnp.zeros((SUBL, LANES), F32), jnp.int32(-1)))
    for lane in range(SUBL):
        out_ref[:, lane * LANES:(lane + 1) * LANES] = acc[pl.ds(lane, out_rows, stride=SUBL), :]


def table_scatter(rows, perm, sid, bst, n_rows, out_rows):
    total = rows.shape[0]
    width = SUBL * LANES
    group, slots = 16, 16
    grid_spec = pltpu.PrefetchScalarGridSpec(
        num_scalar_prefetch=3,
        grid=(n_rows // out_rows,),
        in_specs=[pl.BlockSpec(memory_space=pl.ANY)],
        out_specs=pl.BlockSpec((out_rows, width), lambda b, *_: (b, 0)),
        scratch_shapes=[pltpu.VMEM((out_rows * SUBL + SUBL, LANES), F32), pltpu.VMEM((group * slots, SUBL, LANES), F32), pltpu.SemaphoreType.DMA((slots,))],
    )
    return pl.pallas_call(
        functools.partial(scatter_body, group, slots, out_rows),
        grid_spec=grid_spec,
        out_shape=jax.ShapeDtypeStruct((n_rows, width), F32),
        compiler_params=pltpu.CompilerParams(dimension_semantics=("arbitrary",), vmem_limit_bytes=32 * 1024 * 1024),
        cost_estimate=pl.CostEstimate(flops=70_000_000_000, bytes_accessed=n_rows * width * 4 + total * width * 4, transcendentals=0),
        name="table_scatter",
    )(perm, sid, bst, rows)


def head_prep(raw, gain, cos_t, sin_t):
    values = raw.astype(F32)
    inv = lax.rsqrt(jnp.mean(values * values, axis=-1, keepdims=True) + NORM_EPS)
    normed = values * inv
    scaled = normed * gain
    rot = scaled * cos_t + pltpu.roll(scaled, LANES // 2, 1) * sin_t
    return rot.astype(BF16), normed, inv


def head_prep_bwd(grad, normed, inv, gain, cos_t, sin_t):
    grad_t = grad * cos_t - pltpu.roll(grad, LANES // 2, 1) * sin_t
    grad_gain = jnp.sum(grad_t * normed, axis=0, keepdims=True)
    grad_n = grad_t * gain
    mean_term = jnp.mean(grad_n * normed, axis=-1, keepdims=True)
    return (inv * (grad_n - normed * mean_term)).astype(BF16), grad_gain


def exp_scaled(scores, peak):
    return jnp.exp2((scores - peak) * (LANES ** -0.5 * math.log2(math.e)))


def probs_by_key(q_rot, k_rot, tri):
    h = tri.shape[0]
    top = dot_nt(k_rot[:h], q_rot)
    s_ll = jnp.where(tri, top[:, :h], -1e30)
    s_lh = top[:, h:]
    s_hh = jnp.where(tri, dot_nt(k_rot[h:], q_rot[h:]), -1e30)
    peak_l = jnp.max(s_ll, axis=0, keepdims=True)
    peak_h = jnp.maximum(jnp.max(s_lh, axis=0, keepdims=True), jnp.max(s_hh, axis=0, keepdims=True))
    e_ll, e_lh, e_hh = exp_scaled(s_ll, peak_l), exp_scaled(s_lh, peak_h), exp_scaled(s_hh, peak_h)
    r_l = 1.0 / jnp.sum(e_ll, axis=0, keepdims=True)
    r_h = 1.0 / (jnp.sum(e_lh, axis=0, keepdims=True) + jnp.sum(e_hh, axis=0, keepdims=True))
    return e_ll * r_l, e_lh * r_h, e_hh * r_h


def causal_by_key(seq):
    h = seq // 2
    return lax.broadcasted_iota(jnp.int32, (h, h), 0) <= lax.broadcasted_iota(jnp.int32, (h, h), 1)


def col(start, width):
    return pl.ds(pl.multiple_of(start, LANES), width)


KV_UNROLL = 2


def attn_fwd_body(kv_heads, rep, aliased, *refs):
    if aliased:
        refs = refs[:5] + refs[6:]
    qkv_ref, cos_ref, sin_ref, qn_ref, kn_ref, out_ref = refs
    cos_t, sin_t = cos_ref[...], sin_ref[...]
    q_gain, k_gain = qn_ref[...], kn_ref[...]
    tri = causal_by_key(qkv_ref.shape[0])
    h = tri.shape[0]
    k_base = kv_heads * rep * LANES
    v_base = k_base + kv_heads * LANES

    def per_kv(it, carry):
        for step in range(KV_UNROLL):
            g = it * KV_UNROLL + step
            k_rot, _, _ = head_prep(qkv_ref[:, col(k_base + g * LANES, LANES)], k_gain, cos_t, sin_t)
            v_raw = qkv_ref[:, col(v_base + g * LANES, LANES)]
            for r in range(rep):
                q_rot, _, _ = head_prep(qkv_ref[:, col((g * rep + r) * LANES, LANES)], q_gain, cos_t, sin_t)
                p_ll, p_lh, p_hh = [p.astype(BF16) for p in probs_by_key(q_rot, k_rot, tri)]
                at = col((r * kv_heads + g) * LANES, LANES)
                out_ref[:h, at] = dot_tn(p_ll, v_raw[:h]).astype(BF16)
                out_ref[h:, at] = dot_tn(jnp.concatenate([p_lh, p_hh], axis=0), v_raw).astype(BF16)
        return carry

    lax.fori_loop(0, kv_heads // KV_UNROLL, per_kv, 0)


def attn_bwd_body(kv_heads, rep, n_lead, lead_ref, tail_ref, do_ref, cos_ref, sin_ref, qn_ref, kn_ref, dqkv_ref, dqn_ref, dkn_ref):
    cos_t, sin_t = cos_ref[...], sin_ref[...]
    q_gain, k_gain = qn_ref[...], kn_ref[...]
    tri = causal_by_key(do_ref.shape[0])
    h = tri.shape[0]
    k_base = kv_heads * rep * LANES
    v_base = k_base + kv_heads * LANES
    scale = LANES ** -0.5

    @pl.when(pl.program_id(0) == 0)
    def _():
        dqn_ref[...] = jnp.zeros(dqn_ref.shape, F32)
        dkn_ref[...] = jnp.zeros(dkn_ref.shape, F32)

    def one_seq(qkv_ref):
        def one_kv(g, dqn, dkn):
            k_at = col(k_base + g * LANES, LANES)
            v_at = col(v_base + g * LANES, LANES)
            k_rot, k_normed, k_inv = head_prep(qkv_ref[:, k_at], k_gain, cos_t, sin_t)
            v_raw = qkv_ref[:, v_at]
            dk_l, dk_h, dv_l, dv_h = [], [], [], []
            for r in range(rep):
                at = col((g * rep + r) * LANES, LANES)
                q_rot, q_normed, q_inv = head_prep(qkv_ref[:, at], q_gain, cos_t, sin_t)
                grad_o = do_ref[:, col((r * kv_heads + g) * LANES, LANES)]
                p_ll, p_lh, p_hh = probs_by_key(q_rot, k_rot, tri)
                g_top = dot_nt(v_raw[:h], grad_o)
                g_ll, g_lh = g_top[:, :h], g_top[:, h:]
                g_hh = dot_nt(v_raw[h:], grad_o[h:])
                t_l = jnp.sum(g_ll * p_ll, axis=0, keepdims=True)
                t_h = jnp.sum(g_lh * p_lh, axis=0, keepdims=True) + jnp.sum(g_hh * p_hh, axis=0, keepdims=True)
                s_ll = (p_ll * ((g_ll - t_l) * scale)).astype(BF16)
                s_lh = (p_lh * ((g_lh - t_h) * scale)).astype(BF16)
                s_hh = (p_hh * ((g_hh - t_h) * scale)).astype(BF16)
                dv_l.append(dot_nn(jnp.concatenate([p_ll.astype(BF16), p_lh.astype(BF16)], axis=1), grad_o))
                dv_h.append(dot_nn(p_hh.astype(BF16), grad_o[h:]))
                dk_l.append(dot_nn(jnp.concatenate([s_ll, s_lh], axis=1), q_rot))
                dk_h.append(dot_nn(s_hh, q_rot[h:]))
                dq = jnp.concatenate([dot_tn(s_ll, k_rot[:h]), dot_tn(jnp.concatenate([s_lh, s_hh], axis=0), k_rot)], axis=0)
                dq_raw, gain_part = head_prep_bwd(dq, q_normed, q_inv, q_gain, cos_t, sin_t)
                dqn = dqn + gain_part
                dqkv_ref[:, at] = dq_raw
            dk = jnp.concatenate([sum(dk_l[1:], dk_l[0]), sum(dk_h[1:], dk_h[0])], axis=0)
            dk_raw, gain_part = head_prep_bwd(dk, k_normed, k_inv, k_gain, cos_t, sin_t)
            dkn = dkn + gain_part
            dqkv_ref[:, k_at] = dk_raw
            dqkv_ref[:h, v_at] = sum(dv_l[1:], dv_l[0]).astype(BF16)
            dqkv_ref[h:, v_at] = sum(dv_h[1:], dv_h[0]).astype(BF16)
            return dqn, dkn

        def per_kv(it, carry):
            for step in range(KV_UNROLL):
                carry = one_kv(it * KV_UNROLL + step, *carry)
            return carry

        zero = jnp.zeros((1, LANES), F32)
        dqn, dkn = lax.fori_loop(0, kv_heads // KV_UNROLL, per_kv, (zero, zero))
        dqn_ref[0:1, :] += dqn
        dkn_ref[0:1, :] += dkn

    @pl.when(pl.program_id(0) < n_lead)
    def _():
        one_seq(lead_ref)

    @pl.when(pl.program_id(0) >= n_lead)
    def _():
        one_seq(tail_ref)


def attn_fwd(qkv, cos_t, sin_t, q_gain, k_gain, n_seq, seq, kv_heads, rep, first, into):
    tokens, width = qkv.shape
    q_width = kv_heads * rep * LANES
    own = lambda w: pl.BlockSpec((seq, w), lambda b: (b, 0))
    shifted = lambda w: pl.BlockSpec((seq, w), lambda b: (b + first, 0))
    one = lambda r, w: pl.BlockSpec((r, w), lambda b: (0, 0))
    in_specs = [own(width), shifted(LANES), shifted(LANES), one(1, LANES), one(1, LANES)]
    args = (qkv, cos_t, sin_t, q_gain, k_gain)
    aliases = {}
    if into is not None:
        in_specs.append(pl.BlockSpec(memory_space=pl.ANY))
        args += (into,)
        aliases = {5: 0}
    return pl.pallas_call(
        functools.partial(attn_fwd_body, kv_heads, rep, into is not None),
        grid=(tokens // seq,),
        in_specs=in_specs,
        out_specs=shifted(q_width),
        out_shape=jax.ShapeDtypeStruct((n_seq * seq, q_width), BF16),
        input_output_aliases=aliases,
        compiler_params=pltpu.CompilerParams(dimension_semantics=("arbitrary",), vmem_limit_bytes=32 * 1024 * 1024),
        cost_estimate=pl.CostEstimate(flops=25_000_000_000, bytes_accessed=tokens * (width + q_width) * 2, transcendentals=4_200_000),
        name="attn_fwd",
    )(*args)


def attn_bwd(lead, tail, grad_o, cos_t, sin_t, q_gain, k_gain, seq, kv_heads, rep):
    tokens, q_width = grad_o.shape
    width = lead.shape[1]
    n_lead = lead.shape[0] // seq
    row = lambda w: pl.BlockSpec((seq, w), lambda b: (b, 0))
    one = lambda r, w: pl.BlockSpec((r, w), lambda b: (0, 0))
    lead_spec = pl.BlockSpec((seq, width), lambda b: (jnp.minimum(b, n_lead - 1), 0))
    tail_spec = pl.BlockSpec((seq, width), lambda b: (jnp.maximum(b - n_lead, 0), 0))
    return pl.pallas_call(
        functools.partial(attn_bwd_body, kv_heads, rep, n_lead),
        grid=(tokens // seq,),
        in_specs=[lead_spec, tail_spec, row(q_width), row(LANES), row(LANES), one(1, LANES), one(1, LANES)],
        out_specs=[row(width), one(SUBL, LANES), one(SUBL, LANES)],
        out_shape=[jax.ShapeDtypeStruct((tokens, width), BF16), jax.ShapeDtypeStruct((SUBL, LANES), F32), jax.ShapeDtypeStruct((SUBL, LANES), F32)],
        compiler_params=pltpu.CompilerParams(dimension_semantics=("arbitrary",), vmem_limit_bytes=40 * 1024 * 1024),
        cost_estimate=pl.CostEstimate(flops=100_000_000_000, bytes_accessed=tokens * (2 * width + q_width) * 2, transcendentals=8_400_000),
        name="attn_bwd",
    )(lead, tail, grad_o, cos_t, sin_t, q_gain, k_gain)


FF_TILE = 512
ROW_TILE = 1024
SUB_ROWS = 256


def swiglu_fwd_body(x_ref, w_ref, gu_ref, act_ref):
    for s in range(0, x_ref.shape[0], SUB_ROWS):
        rows = slice(s, s + SUB_ROWS)
        both = dot_nn(x_ref[rows, :], w_ref[...])
        gu_ref[rows, :] = both
        gate, up = both[:, :FF_TILE], both[:, FF_TILE:]
        act_ref[rows, :] = (gate * jax.nn.sigmoid(gate) * up).astype(BF16)


def swiglu_fwd(x, w_gu):
    tokens, dim = x.shape
    both = w_gu.shape[1]
    ff = both // 2
    return pl.pallas_call(
        swiglu_fwd_body,
        grid=(ff // FF_TILE, tokens // ROW_TILE),
        in_specs=[pl.BlockSpec((ROW_TILE, dim), lambda n, m: (m, 0)), pl.BlockSpec((dim, 2 * FF_TILE), lambda n, m: (0, n))],
        out_specs=[pl.BlockSpec((ROW_TILE, 2 * FF_TILE), lambda n, m: (m, n)), pl.BlockSpec((ROW_TILE, FF_TILE), lambda n, m: (m, n))],
        out_shape=[jax.ShapeDtypeStruct((tokens, both), F32), jax.ShapeDtypeStruct((tokens, ff), BF16)],
        compiler_params=pltpu.CompilerParams(dimension_semantics=("arbitrary", "arbitrary"), vmem_limit_bytes=40 * 1024 * 1024),
        cost_estimate=pl.CostEstimate(flops=2 * tokens * dim * both, bytes_accessed=tokens * both * 5, transcendentals=tokens * ff),
        name="swiglu_fwd",
    )(x, w_gu)


def swiglu_bwd_body(dy_ref, w_ref, gu_ref, dgu_ref):
    for s in range(0, dy_ref.shape[0], SUB_ROWS):
        rows = slice(s, s + SUB_ROWS)
        grad_act = dot_nt(dy_ref[rows, :], w_ref[...])
        gate, up = gu_ref[rows, :FF_TILE], gu_ref[rows, FF_TILE:]
        sig = jax.nn.sigmoid(gate)
        part = grad_act * sig
        dgu_ref[rows, :FF_TILE] = (part * up * (1.0 + gate * (1.0 - sig))).astype(BF16)
        dgu_ref[rows, FF_TILE:] = (part * gate).astype(BF16)


def swiglu_bwd(dy, w_down, gu):
    tokens, dim = dy.shape
    ff = w_down.shape[0]
    return pl.pallas_call(
        swiglu_bwd_body,
        grid=(ff // FF_TILE, tokens // ROW_TILE),
        in_specs=[pl.BlockSpec((ROW_TILE, dim), lambda n, m: (m, 0)), pl.BlockSpec((FF_TILE, dim), lambda n, m: (n, 0)), pl.BlockSpec((ROW_TILE, 2 * FF_TILE), lambda n, m: (m, n))],
        out_specs=pl.BlockSpec((ROW_TILE, 2 * FF_TILE), lambda n, m: (m, n)),
        out_shape=jax.ShapeDtypeStruct((tokens, 2 * ff), BF16),
        compiler_params=pltpu.CompilerParams(dimension_semantics=("arbitrary", "arbitrary"), vmem_limit_bytes=40 * 1024 * 1024),
        cost_estimate=pl.CostEstimate(flops=2 * tokens * dim * ff, bytes_accessed=tokens * ff * 12, transcendentals=tokens * ff),
        name="swiglu_bwd",
    )(dy, w_down, gu)


def norm_grad_body(as_rows, sub, g_ref, w_ref, x_ref, res_ref, gain_ref, *outs):
    gain = gain_ref[...]
    dgain_ref = outs[-1]

    @pl.when(pl.program_id(0) == 0)
    def _():
        dgain_ref[...] = jnp.zeros(dgain_ref.shape, F32)

    total = jnp.zeros(gain.shape, F32)
    for s in range(0, g_ref.shape[0], sub):
        rows = slice(s, s + sub)
        grad = dot_nt(g_ref[rows, :], w_ref[...])
        values = x_ref[rows, :].astype(F32)
        inv = lax.rsqrt(jnp.mean(values * values, axis=-1, keepdims=True) + NORM_EPS)
        normed = values * inv
        total = total + jnp.sum(grad * normed, axis=0, keepdims=True)
        scaled = grad * gain
        mean_term = jnp.mean(scaled * normed, axis=-1, keepdims=True)
        result = res_ref[rows, :].astype(F32) + inv * (scaled - normed * mean_term)
        if as_rows:
            for lane in range(SUBL):
                outs[0][pl.ds(s * SUBL + lane, sub, stride=SUBL), :] = result[:, lane * LANES:(lane + 1) * LANES]
        else:
            outs[0][rows, :] = result
            outs[1][rows, :] = result.astype(BF16)
    dgain_ref[0:1, :] += total


def norm_grad(g, w, x, residual, gain, as_rows):
    tokens, width = g.shape
    dim = w.shape[0]
    tile, sub = 512, 256
    row = lambda w: pl.BlockSpec((tile, w), lambda m: (m, 0))
    one = lambda r, w: pl.BlockSpec((r, w), lambda m: (0, 0))
    if as_rows:
        out_specs = [pl.BlockSpec((tile * SUBL, LANES), lambda m: (m, 0))]
        out_shape = [jax.ShapeDtypeStruct((tokens * SUBL, LANES), F32)]
    else:
        out_specs = [row(dim), row(dim)]
        out_shape = [jax.ShapeDtypeStruct((tokens, dim), F32), jax.ShapeDtypeStruct((tokens, dim), BF16)]
    return pl.pallas_call(
        functools.partial(norm_grad_body, as_rows, sub),
        grid=(tokens // tile,),
        in_specs=[row(width), pl.BlockSpec((dim, width), lambda m: (0, 0), pipeline_mode=pl.Buffered(1)), row(dim), row(dim), one(1, dim)],
        out_specs=out_specs + [one(SUBL, dim)],
        out_shape=out_shape + [jax.ShapeDtypeStruct((SUBL, dim), F32)],
        compiler_params=pltpu.CompilerParams(dimension_semantics=("arbitrary",), vmem_limit_bytes=VMEM_LIMIT),
        cost_estimate=pl.CostEstimate(flops=2 * tokens * dim * width, bytes_accessed=2 * tokens * width + 2 * dim * width + 12 * tokens * dim, transcendentals=0),
    )(g, w, x, residual, gain)


def norm_fwd(values):
    values_f = values.astype(F32)
    inv_rms = lax.rsqrt(jnp.mean(values_f * values_f, axis=-1, keepdims=True) + NORM_EPS)
    return values_f * inv_rms, inv_rms


def gather_rows(shard):
    return lax.all_gather(shard, AXIS_NAME, tiled=True)


def scatter_rows(grad):
    return lax.psum_scatter(grad, AXIS_NAME, scatter_dimension=0, tiled=True)


def side_by_side(gate, up):
    rows, ff = gate.shape
    tiles = ff // FF_TILE
    both = jnp.stack([gate.reshape(rows, tiles, FF_TILE), up.reshape(rows, tiles, FF_TILE)], axis=2)
    return both.reshape(rows, 2 * ff)


def take_apart(both):
    rows, width = both.shape
    parts = both.reshape(rows, width // (2 * FF_TILE), 2, FF_TILE)
    return parts[:, :, 0].reshape(rows, width // 2), parts[:, :, 1].reshape(rows, width // 2)


def solution(mesh):
    row_spec = P(AXIS_NAME, None)
    vec_spec = P(AXIS_NAME)
    full_spec = P(None)
    batch_spec = P(AXIS_NAME, None, None)
    weight_specs = (vec_spec, row_spec, row_spec, row_spec, full_spec, full_spec, row_spec, vec_spec, row_spec, row_spec, row_spec)

    def device_step(tokens, positions, table, attn_norm, w_query, w_key, w_value, q_norm, k_norm, w_out, mlp_norm, w_gate, w_up, w_down, dy_out):
        n_seq, seq = tokens.shape
        n_tok = n_seq * seq
        rows_local, dim = table.shape
        head = q_norm.shape[0]
        kv_heads = w_key.shape[1] // head
        rep = w_query.shape[1] // w_key.shape[1]
        q_width, kv_width = w_query.shape[1], w_key.shape[1]

        all_ids = gather_rows(tokens.reshape(-1))
        n_dev = all_ids.shape[0] // n_tok
        local_ids = all_ids - lax.axis_index(AXIS_NAME) * rows_local
        is_owner = (local_ids >= 0) & (local_ids < rows_local)
        owned_ids = jnp.where(is_owner, local_ids, rows_local)

        w_qkv = gather_rows(jnp.concatenate([w_query, w_key, w_value], axis=1))
        out_half = w_out.shape[0] // 2
        w_o = gather_rows(jnp.concatenate([w_out[:out_half], w_out[out_half:]], axis=1))
        n_lead = 5 * n_seq // 8
        lead_tok = n_lead * seq
        by_dev = owned_ids.reshape(n_dev, n_tok)
        ordered = jnp.concatenate([by_dev[:, :lead_tok].reshape(-1), by_dev[:, lead_tok:].reshape(-1)])
        picked_a, picked_b = table_gather(table, ordered, n_dev * lead_tok)
        x_a = scatter_rows(picked_a).reshape(lead_tok, dim)
        x_b = scatter_rows(picked_b).reshape(n_tok - lead_tok, dim)

        gu_local, down_local, norms_local, _ = lax.optimization_barrier((side_by_side(w_gate, w_up), w_down, jnp.stack([attn_norm, mlp_norm]), picked_b))
        w_gu = gather_rows(gu_local)
        w_d = gather_rows(down_local)
        norms = lax.all_gather(norms_local, AXIS_NAME, axis=1, tiled=True).astype(F32)
        attn_gain, mlp_gain = norms[0][None], norms[1][None]

        sid, perm = lax.sort([owned_ids, lax.iota(jnp.int32, all_ids.shape[0])], num_keys=1, is_stable=False)
        out_rows = block_of(rows_local, 300, SUBL)
        edges = lax.iota(jnp.int32, rows_local // out_rows + 1) * out_rows
        bst = jnp.sum((owned_ids[None, :] < edges[:, None]).astype(jnp.int32), axis=1)

        half = head // 2
        inv_freq = jnp.exp(jnp.arange(half, dtype=F32) * (-2.0 * math.log(ROPE_THETA) / head))
        angles = positions.reshape(-1).astype(F32)[:, None] * inv_freq
        cos_h, sin_h = jnp.cos(angles), jnp.sin(angles)
        cos_t = jnp.concatenate([cos_h, cos_h], axis=1)
        sin_t = jnp.concatenate([-sin_h, sin_h], axis=1)
        q_gain = q_norm.astype(F32)[None]
        k_gain = k_norm.astype(F32)[None]

        w_o = jnp.concatenate([w_o[:, :dim], w_o[:, dim:]], axis=0)

        def attn_norm_of(x_part):
            normed, _ = norm_fwd(x_part)
            return (normed * attn_gain).astype(BF16)

        qkv_a = dot_nn(attn_norm_of(x_a), w_qkv).astype(BF16)
        heads = attn_fwd(qkv_a, cos_t, sin_t, q_gain, k_gain, n_seq, seq, kv_heads, rep, 0, None)
        qkv_b = dot_nn(attn_norm_of(x_b), w_qkv).astype(BF16)
        heads = attn_fwd(qkv_b, cos_t, sin_t, q_gain, k_gain, n_seq, seq, kv_heads, rep, n_lead, heads)
        x_a, x_b, heads = lax.optimization_barrier((x_a, x_b, heads))
        x_emb = jnp.concatenate([x_a, x_b])
        hidden = (x_emb.astype(F32) + dot_nn(heads, w_o)).astype(BF16)
        normed2, _ = norm_fwd(hidden)
        mlp_in = (normed2 * mlp_gain).astype(BF16)
        gu, act = swiglu_fwd(mlp_in, w_gu)
        dy = dy_out.reshape(n_tok, dim)

        down_full, dy_later = lax.optimization_barrier((dot_tn(act, dy), dy))
        d_down = scatter_rows(down_full)
        dgu = swiglu_bwd(dy_later, w_d, gu)
        gu_full, dgu = lax.optimization_barrier((dot_tn(mlp_in, dgu), dgu))
        d_gu = scatter_rows(gu_full)
        grad_hidden, hidden_b, d_mlp_norm = norm_grad(dgu, w_gu, hidden, dy, mlp_gain, False)
        grad_heads = dot_nt(hidden_b, w_o).astype(BF16)
        dqkv, dqn, dkn = attn_bwd(qkv_a, qkv_b, grad_heads, cos_t, sin_t, q_gain, k_gain, seq, kv_heads, rep)
        grad_x, d_attn_norm = norm_grad(dqkv, w_qkv, x_emb, grad_hidden, attn_gain, True)
        grad_x = grad_x.reshape(n_tok, SUBL, LANES)
        grad_x, dqkv, act_later, hidden_later, x_later = lax.optimization_barrier((grad_x, dqkv, act, hidden_b, x_emb))
        all_rows = gather_rows(grad_x)
        d_out_full = dot_tn(heads, hidden_later)
        mid = d_out_full.shape[0] // 2
        d_qkvo = scatter_rows(jnp.concatenate([dot_tn(attn_norm_of(x_later), dqkv), d_out_full[:mid], d_out_full[mid:]], axis=1))
        layer_out = (hidden.astype(F32) + dot_nn(act_later, w_d)).astype(BF16)

        small = lax.psum(jnp.concatenate([d_attn_norm[0], d_mlp_norm[0], dqn[0], dkn[0]]), AXIS_NAME)
        shard_len = attn_norm.shape[0]
        at = lax.axis_index(AXIS_NAME) * shard_len
        d_attn_norm = lax.dynamic_slice(small, (at,), (shard_len,))
        d_mlp_norm = lax.dynamic_slice(small, (dim + at,), (shard_len,))
        d_q_norm = small[2 * dim:2 * dim + head]
        d_k_norm = small[2 * dim + head:]

        d_table = table_scatter(all_rows, perm, sid, bst, rows_local, out_rows)
        d_gate, d_up = take_apart(d_gu)
        cuts = [q_width, q_width + kv_width, q_width + 2 * kv_width, q_width + 2 * kv_width + dim]
        d_query, d_key, d_value, out_even, out_odd = jnp.split(d_qkvo, cuts, axis=1)
        d_out = jnp.concatenate([out_even, out_odd], axis=0)
        return (layer_out.reshape(n_seq, seq, dim), d_table, d_attn_norm, d_query, d_key, d_value, d_q_norm, d_k_norm, d_out, d_mlp_norm, d_gate, d_up, d_down)

    return jax.shard_map(device_step, mesh=mesh, in_specs=(row_spec, row_spec, row_spec) + weight_specs + (batch_spec,), out_specs=(batch_spec, row_spec) + weight_specs, check_vma=False)
```

```python
import functools
import math
import jax
import jax.numpy as jnp
from jax import lax
from jax.experimental import pallas as pl
from jax.experimental.pallas import tpu as pltpu
from jax.sharding import PartitionSpec as P

NORM_EPS = 1e-6
ROPE_THETA = 1.0e6
AXIS_NAME = 'fsdp'
F32 = jnp.float32
BF16 = jnp.bfloat16
LANES = 128
SUBL = 8
VMEM_LIMIT = 60 * 1024 * 1024


def dot_nt(a, b):
    return lax.dot_general(a, b, (((1,), (1,)), ((), ())), preferred_element_type=F32)


def dot_tn(a, b):
    return lax.dot_general(a, b, (((0,), (0,)), ((), ())), preferred_element_type=F32)


def dot_nn(a, b):
    return jnp.dot(a, b, preferred_element_type=F32)


def block_of(total, limit, step):
    best = step
    for size in range(step, limit + 1, step):
        if total % size == 0:
            best = size
    return best


def gather_body(n_tab, starts, tab_rows, tok_rows, idx_ref, tab_ref, *refs):
    out_refs, (store, stage) = refs[:-2], refs[-2:]
    step = pl.program_id(0)

    @pl.when(step == 0)
    def _():
        store[n_tab * tab_rows] = jnp.zeros((SUBL, LANES), BF16)

    @pl.when(step < n_tab)
    def _():
        for lane in range(SUBL):
            stage[pl.ds(lane, tab_rows, stride=SUBL), :] = tab_ref[:, lane * LANES:(lane + 1) * LANES].astype(F32)
        rows = stage[...].reshape(tab_rows, SUBL, LANES)
        store[pl.ds(step * tab_rows, tab_rows)] = rows.astype(BF16)

    def copy_rows(out_ref):
        base = (step - n_tab) * tok_rows
        unroll = 16

        def loop(it, carry):
            first = it * unroll
            for u in range(unroll):
                out_ref[first + u] = store[idx_ref[base + first + u]]
            return carry

        lax.fori_loop(0, tok_rows // unroll, loop, 0)

    for k, out_ref in enumerate(out_refs):
        @pl.when((step >= n_tab + starts[k]) & (step < n_tab + starts[k + 1]))
        def _(out_ref=out_ref):
            copy_rows(out_ref)


def table_gather(table, idx, counts):
    rows, width = table.shape
    tab_rows = block_of(rows, 640, 16)
    n_tab = rows // tab_rows
    tok_rows = 512
    starts = [sum(counts[:k]) // tok_rows for k in range(len(counts) + 1)]
    out_spec = lambda lo, hi: pl.BlockSpec((tok_rows, SUBL, LANES), lambda s, ids: (jnp.clip(s - n_tab - lo, 0, hi - lo - 1), 0, 0))
    grid_spec = pltpu.PrefetchScalarGridSpec(
        num_scalar_prefetch=1,
        grid=(n_tab + starts[-1],),
        in_specs=[pl.BlockSpec((tab_rows, width), lambda s, ids: (jnp.minimum(s, n_tab - 1), 0))],
        out_specs=[out_spec(lo, hi) for lo, hi in zip(starts, starts[1:])],
        scratch_shapes=[pltpu.VMEM((rows + 8, SUBL, LANES), BF16), pltpu.VMEM((tab_rows * SUBL, LANES), F32)],
    )
    return pl.pallas_call(
        functools.partial(gather_body, n_tab, starts, tab_rows, tok_rows),
        grid_spec=grid_spec,
        out_shape=[jax.ShapeDtypeStruct((n, SUBL, LANES), BF16) for n in counts],
        compiler_params=pltpu.CompilerParams(dimension_semantics=("arbitrary",), vmem_limit_bytes=VMEM_LIMIT),
        cost_estimate=pl.CostEstimate(flops=70_000_000_000, bytes_accessed=rows * width * 2 + sum(counts) * width * 2, transcendentals=0),
        name="table_gather",
    )(idx, table)


def scatter_body(group, slots, out_rows, perm_ref, sid_ref, bst_ref, rows_ref, out_ref, acc, ring, sem):
    blk = pl.program_id(0)
    total = bst_ref[pl.num_programs(0)]
    n_groups = (total + group - 1) // group

    def issue(g):
        slot = lax.rem(g, slots)
        for u in range(group):
            pltpu.make_async_copy(rows_ref.at[perm_ref[g * group + u]], ring.at[slot * group + u], sem.at[slot]).start()

    @pl.when(blk == 0)
    def _():
        def first(g, carry):
            issue(g)
            return carry

        lax.fori_loop(0, jnp.minimum(n_groups, slots), first, 0)

    acc[...] = jnp.zeros(acc.shape, F32)
    low = bst_ref[blk]
    high = bst_ref[blk + 1]
    g_first = low // group
    g_last = jnp.where(high > low, (high + group - 1) // group, g_first)
    base = blk * out_rows

    def per_group(g, carry):
        start = g * group
        slot = lax.rem(g, slots)

        @pl.when(start >= low)
        def _():
            pltpu.make_async_copy(rows_ref.at[pl.ds(0, group)], ring.at[pl.ds(slot * group, group)], sem.at[slot]).wait()

        prev, prev_id = carry
        for u in range(group):
            row_id = sid_ref[start + u]
            local = row_id - base
            inside = (local >= 0) & (local < out_rows)
            value = ring[slot * group + u]
            value = jnp.where(row_id == prev_id, prev + value, value)
            acc[pl.ds(pl.multiple_of(jnp.where(inside, local, out_rows) * SUBL, SUBL), SUBL), :] = value
            prev, prev_id = value, row_id

        @pl.when((high >= start + group) & (g + slots < n_groups))
        def _():
            issue(g + slots)

        return prev, prev_id

    lax.fori_loop(g_first, g_last, per_group, (jnp.zeros((SUBL, LANES), F32), jnp.int32(-1)))
    for lane in range(SUBL):
        out_ref[:, lane * LANES:(lane + 1) * LANES] = acc[pl.ds(lane, out_rows, stride=SUBL), :]


def table_scatter(rows, perm, sid, bst, n_rows, out_rows):
    total = rows.shape[0]
    width = SUBL * LANES
    group, slots = 16, 16
    grid_spec = pltpu.PrefetchScalarGridSpec(
        num_scalar_prefetch=3,
        grid=(n_rows // out_rows,),
        in_specs=[pl.BlockSpec(memory_space=pl.ANY)],
        out_specs=pl.BlockSpec((out_rows, width), lambda b, *_: (b, 0)),
        scratch_shapes=[pltpu.VMEM((out_rows * SUBL + SUBL, LANES), F32), pltpu.VMEM((group * slots, SUBL, LANES), F32), pltpu.SemaphoreType.DMA((slots,))],
    )
    return pl.pallas_call(
        functools.partial(scatter_body, group, slots, out_rows),
        grid_spec=grid_spec,
        out_shape=jax.ShapeDtypeStruct((n_rows, width), F32),
        compiler_params=pltpu.CompilerParams(dimension_semantics=("arbitrary",), vmem_limit_bytes=32 * 1024 * 1024),
        cost_estimate=pl.CostEstimate(flops=70_000_000_000, bytes_accessed=n_rows * width * 4 + total * width * 4, transcendentals=0),
        name="table_scatter",
    )(perm, sid, bst, rows)


def head_prep(raw, gain, cos_t, sin_t):
    values = raw.astype(F32)
    inv = lax.rsqrt(jnp.mean(values * values, axis=-1, keepdims=True) + NORM_EPS)
    normed = values * inv
    scaled = normed * gain
    rot = scaled * cos_t + pltpu.roll(scaled, LANES // 2, 1) * sin_t
    return rot.astype(BF16), normed, inv


def head_prep_bwd(grad, normed, inv, gain, cos_t, sin_t):
    grad_t = grad * cos_t - pltpu.roll(grad, LANES // 2, 1) * sin_t
    grad_gain = jnp.sum(grad_t * normed, axis=0, keepdims=True)
    grad_n = grad_t * gain
    mean_term = jnp.mean(grad_n * normed, axis=-1, keepdims=True)
    return (inv * (grad_n - normed * mean_term)).astype(BF16), grad_gain


def exp_scaled(scores, peak):
    return jnp.exp2((scores - peak) * (LANES ** -0.5 * math.log2(math.e)))


def probs_by_key(q_rot, k_rot, tri):
    h = tri.shape[0]
    top = dot_nt(k_rot[:h], q_rot)
    s_ll = jnp.where(tri, top[:, :h], -1e30)
    s_lh = top[:, h:]
    s_hh = jnp.where(tri, dot_nt(k_rot[h:], q_rot[h:]), -1e30)
    peak_l = jnp.max(s_ll, axis=0, keepdims=True)
    peak_h = jnp.maximum(jnp.max(s_lh, axis=0, keepdims=True), jnp.max(s_hh, axis=0, keepdims=True))
    e_ll, e_lh, e_hh = exp_scaled(s_ll, peak_l), exp_scaled(s_lh, peak_h), exp_scaled(s_hh, peak_h)
    r_l = 1.0 / jnp.sum(e_ll, axis=0, keepdims=True)
    r_h = 1.0 / (jnp.sum(e_lh, axis=0, keepdims=True) + jnp.sum(e_hh, axis=0, keepdims=True))
    return e_ll * r_l, e_lh * r_h, e_hh * r_h


def causal_by_key(seq):
    h = seq // 2
    return lax.broadcasted_iota(jnp.int32, (h, h), 0) <= lax.broadcasted_iota(jnp.int32, (h, h), 1)


def col(start, width):
    return pl.ds(pl.multiple_of(start, LANES), width)


KV_UNROLL = 2


def attn_fwd_body(kv_heads, rep, aliased, *refs):
    if aliased:
        refs = refs[:5] + refs[6:]
    qkv_ref, cos_ref, sin_ref, qn_ref, kn_ref, out_ref = refs
    cos_t, sin_t = cos_ref[...], sin_ref[...]
    q_gain, k_gain = qn_ref[...], kn_ref[...]
    tri = causal_by_key(qkv_ref.shape[0])
    h = tri.shape[0]
    k_base = kv_heads * rep * LANES
    v_base = k_base + kv_heads * LANES

    def per_kv(it, carry):
        for step in range(KV_UNROLL):
            g = it * KV_UNROLL + step
            k_rot, _, _ = head_prep(qkv_ref[:, col(k_base + g * LANES, LANES)], k_gain, cos_t, sin_t)
            v_raw = qkv_ref[:, col(v_base + g * LANES, LANES)]
            for r in range(rep):
                q_rot, _, _ = head_prep(qkv_ref[:, col((g * rep + r) * LANES, LANES)], q_gain, cos_t, sin_t)
                p_ll, p_lh, p_hh = [p.astype(BF16) for p in probs_by_key(q_rot, k_rot, tri)]
                at = col((r * kv_heads + g) * LANES, LANES)
                out_ref[:h, at] = dot_tn(p_ll, v_raw[:h]).astype(BF16)
                out_ref[h:, at] = dot_tn(jnp.concatenate([p_lh, p_hh], axis=0), v_raw).astype(BF16)
        return carry

    lax.fori_loop(0, kv_heads // KV_UNROLL, per_kv, 0)


def attn_bwd_body(kv_heads, rep, n_lead, lead_ref, tail_ref, do_ref, cos_ref, sin_ref, qn_ref, kn_ref, dqkv_ref, dqn_ref, dkn_ref):
    cos_t, sin_t = cos_ref[...], sin_ref[...]
    q_gain, k_gain = qn_ref[...], kn_ref[...]
    tri = causal_by_key(do_ref.shape[0])
    h = tri.shape[0]
    k_base = kv_heads * rep * LANES
    v_base = k_base + kv_heads * LANES
    scale = LANES ** -0.5

    @pl.when(pl.program_id(0) == 0)
    def _():
        dqn_ref[...] = jnp.zeros(dqn_ref.shape, F32)
        dkn_ref[...] = jnp.zeros(dkn_ref.shape, F32)

    def one_seq(qkv_ref):
        def one_kv(g, dqn, dkn):
            k_at = col(k_base + g * LANES, LANES)
            v_at = col(v_base + g * LANES, LANES)
            k_rot, k_normed, k_inv = head_prep(qkv_ref[:, k_at], k_gain, cos_t, sin_t)
            v_raw = qkv_ref[:, v_at]
            dk_l, dk_h, dv_l, dv_h = [], [], [], []
            for r in range(rep):
                at = col((g * rep + r) * LANES, LANES)
                q_rot, q_normed, q_inv = head_prep(qkv_ref[:, at], q_gain, cos_t, sin_t)
                grad_o = do_ref[:, col((r * kv_heads + g) * LANES, LANES)]
                p_ll, p_lh, p_hh = probs_by_key(q_rot, k_rot, tri)
                g_top = dot_nt(v_raw[:h], grad_o)
                g_ll, g_lh = g_top[:, :h], g_top[:, h:]
                g_hh = dot_nt(v_raw[h:], grad_o[h:])
                t_l = jnp.sum(g_ll * p_ll, axis=0, keepdims=True)
                t_h = jnp.sum(g_lh * p_lh, axis=0, keepdims=True) + jnp.sum(g_hh * p_hh, axis=0, keepdims=True)
                s_ll = (p_ll * ((g_ll - t_l) * scale)).astype(BF16)
                s_lh = (p_lh * ((g_lh - t_h) * scale)).astype(BF16)
                s_hh = (p_hh * ((g_hh - t_h) * scale)).astype(BF16)
                dv_l.append(dot_nn(jnp.concatenate([p_ll.astype(BF16), p_lh.astype(BF16)], axis=1), grad_o))
                dv_h.append(dot_nn(p_hh.astype(BF16), grad_o[h:]))
                dk_l.append(dot_nn(jnp.concatenate([s_ll, s_lh], axis=1), q_rot))
                dk_h.append(dot_nn(s_hh, q_rot[h:]))
                dq = jnp.concatenate([dot_tn(s_ll, k_rot[:h]), dot_tn(jnp.concatenate([s_lh, s_hh], axis=0), k_rot)], axis=0)
                dq_raw, gain_part = head_prep_bwd(dq, q_normed, q_inv, q_gain, cos_t, sin_t)
                dqn = dqn + gain_part
                dqkv_ref[:, at] = dq_raw
            dk = jnp.concatenate([sum(dk_l[1:], dk_l[0]), sum(dk_h[1:], dk_h[0])], axis=0)
            dk_raw, gain_part = head_prep_bwd(dk, k_normed, k_inv, k_gain, cos_t, sin_t)
            dkn = dkn + gain_part
            dqkv_ref[:, k_at] = dk_raw
            dqkv_ref[:h, v_at] = sum(dv_l[1:], dv_l[0]).astype(BF16)
            dqkv_ref[h:, v_at] = sum(dv_h[1:], dv_h[0]).astype(BF16)
            return dqn, dkn

        def per_kv(it, carry):
            for step in range(KV_UNROLL):
                carry = one_kv(it * KV_UNROLL + step, *carry)
            return carry

        zero = jnp.zeros((1, LANES), F32)
        dqn, dkn = lax.fori_loop(0, kv_heads // KV_UNROLL, per_kv, (zero, zero))
        dqn_ref[0:1, :] += dqn
        dkn_ref[0:1, :] += dkn

    @pl.when(pl.program_id(0) < n_lead)
    def _():
        one_seq(lead_ref)

    @pl.when(pl.program_id(0) >= n_lead)
    def _():
        one_seq(tail_ref)


def attn_fwd(qkv, cos_t, sin_t, q_gain, k_gain, n_seq, seq, kv_heads, rep, first, into):
    tokens, width = qkv.shape
    q_width = kv_heads * rep * LANES
    own = lambda w: pl.BlockSpec((seq, w), lambda b: (b, 0))
    shifted = lambda w: pl.BlockSpec((seq, w), lambda b: (b + first, 0))
    one = lambda r, w: pl.BlockSpec((r, w), lambda b: (0, 0))
    in_specs = [own(width), shifted(LANES), shifted(LANES), one(1, LANES), one(1, LANES)]
    args = (qkv, cos_t, sin_t, q_gain, k_gain)
    aliases = {}
    if into is not None:
        in_specs.append(pl.BlockSpec(memory_space=pl.ANY))
        args += (into,)
        aliases = {5: 0}
    return pl.pallas_call(
        functools.partial(attn_fwd_body, kv_heads, rep, into is not None),
        grid=(tokens // seq,),
        in_specs=in_specs,
        out_specs=shifted(q_width),
        out_shape=jax.ShapeDtypeStruct((n_seq * seq, q_width), BF16),
        input_output_aliases=aliases,
        compiler_params=pltpu.CompilerParams(dimension_semantics=("arbitrary",), vmem_limit_bytes=32 * 1024 * 1024),
        cost_estimate=pl.CostEstimate(flops=25_000_000_000, bytes_accessed=tokens * (width + q_width) * 2, transcendentals=4_200_000),
        name="attn_fwd",
    )(*args)


def attn_bwd(lead, tail, grad_o, cos_t, sin_t, q_gain, k_gain, seq, kv_heads, rep):
    tokens, q_width = grad_o.shape
    width = lead.shape[1]
    n_lead = lead.shape[0] // seq
    row = lambda w: pl.BlockSpec((seq, w), lambda b: (b, 0))
    one = lambda r, w: pl.BlockSpec((r, w), lambda b: (0, 0))
    lead_spec = pl.BlockSpec((seq, width), lambda b: (jnp.minimum(b, n_lead - 1), 0))
    tail_spec = pl.BlockSpec((seq, width), lambda b: (jnp.maximum(b - n_lead, 0), 0))
    return pl.pallas_call(
        functools.partial(attn_bwd_body, kv_heads, rep, n_lead),
        grid=(tokens // seq,),
        in_specs=[lead_spec, tail_spec, row(q_width), row(LANES), row(LANES), one(1, LANES), one(1, LANES)],
        out_specs=[row(width), one(SUBL, LANES), one(SUBL, LANES)],
        out_shape=[jax.ShapeDtypeStruct((tokens, width), BF16), jax.ShapeDtypeStruct((SUBL, LANES), F32), jax.ShapeDtypeStruct((SUBL, LANES), F32)],
        compiler_params=pltpu.CompilerParams(dimension_semantics=("arbitrary",), vmem_limit_bytes=40 * 1024 * 1024),
        cost_estimate=pl.CostEstimate(flops=100_000_000_000, bytes_accessed=tokens * (2 * width + q_width) * 2, transcendentals=8_400_000),
        name="attn_bwd",
    )(lead, tail, grad_o, cos_t, sin_t, q_gain, k_gain)


FF_TILE = 512
ROW_TILE = 1024
SUB_ROWS = 256


def swiglu_fwd_body(x_ref, w_ref, gu_ref, act_ref):
    for s in range(0, x_ref.shape[0], SUB_ROWS):
        rows = slice(s, s + SUB_ROWS)
        both = dot_nn(x_ref[rows, :], w_ref[...])
        gu_ref[rows, :] = both
        gate, up = both[:, :FF_TILE], both[:, FF_TILE:]
        act_ref[rows, :] = (gate * jax.nn.sigmoid(gate) * up).astype(BF16)


def swiglu_fwd(x, w_gu):
    tokens, dim = x.shape
    both = w_gu.shape[1]
    ff = both // 2
    return pl.pallas_call(
        swiglu_fwd_body,
        grid=(ff // FF_TILE, tokens // ROW_TILE),
        in_specs=[pl.BlockSpec((ROW_TILE, dim), lambda n, m: (m, 0)), pl.BlockSpec((dim, 2 * FF_TILE), lambda n, m: (0, n))],
        out_specs=[pl.BlockSpec((ROW_TILE, 2 * FF_TILE), lambda n, m: (m, n)), pl.BlockSpec((ROW_TILE, FF_TILE), lambda n, m: (m, n))],
        out_shape=[jax.ShapeDtypeStruct((tokens, both), F32), jax.ShapeDtypeStruct((tokens, ff), BF16)],
        compiler_params=pltpu.CompilerParams(dimension_semantics=("arbitrary", "arbitrary"), vmem_limit_bytes=40 * 1024 * 1024),
        cost_estimate=pl.CostEstimate(flops=2 * tokens * dim * both, bytes_accessed=tokens * both * 5, transcendentals=tokens * ff),
        name="swiglu_fwd",
    )(x, w_gu)


def swiglu_bwd_body(dy_ref, w_ref, gu_ref, dgu_ref):
    for s in range(0, dy_ref.shape[0], SUB_ROWS):
        rows = slice(s, s + SUB_ROWS)
        grad_act = dot_nt(dy_ref[rows, :], w_ref[...])
        gate, up = gu_ref[rows, :FF_TILE], gu_ref[rows, FF_TILE:]
        sig = jax.nn.sigmoid(gate)
        part = grad_act * sig
        dgu_ref[rows, :FF_TILE] = (part * up * (1.0 + gate * (1.0 - sig))).astype(BF16)
        dgu_ref[rows, FF_TILE:] = (part * gate).astype(BF16)


def swiglu_bwd(dy, w_down, gu):
    tokens, dim = dy.shape
    ff = w_down.shape[0]
    return pl.pallas_call(
        swiglu_bwd_body,
        grid=(ff // FF_TILE, tokens // ROW_TILE),
        in_specs=[pl.BlockSpec((ROW_TILE, dim), lambda n, m: (m, 0)), pl.BlockSpec((FF_TILE, dim), lambda n, m: (n, 0)), pl.BlockSpec((ROW_TILE, 2 * FF_TILE), lambda n, m: (m, n))],
        out_specs=pl.BlockSpec((ROW_TILE, 2 * FF_TILE), lambda n, m: (m, n)),
        out_shape=jax.ShapeDtypeStruct((tokens, 2 * ff), BF16),
        compiler_params=pltpu.CompilerParams(dimension_semantics=("arbitrary", "arbitrary"), vmem_limit_bytes=40 * 1024 * 1024),
        cost_estimate=pl.CostEstimate(flops=2 * tokens * dim * ff, bytes_accessed=tokens * ff * 12, transcendentals=tokens * ff),
        name="swiglu_bwd",
    )(dy, w_down, gu)


def norm_grad_body(as_rows, sub, g_ref, w_ref, x_ref, res_ref, gain_ref, *outs):
    gain = gain_ref[...]
    dgain_ref = outs[-1]

    @pl.when(pl.program_id(0) == 0)
    def _():
        dgain_ref[...] = jnp.zeros(dgain_ref.shape, F32)

    total = jnp.zeros(gain.shape, F32)
    for s in range(0, g_ref.shape[0], sub):
        rows = slice(s, s + sub)
        grad = dot_nt(g_ref[rows, :], w_ref[...])
        values = x_ref[rows, :].astype(F32)
        inv = lax.rsqrt(jnp.mean(values * values, axis=-1, keepdims=True) + NORM_EPS)
        normed = values * inv
        total = total + jnp.sum(grad * normed, axis=0, keepdims=True)
        scaled = grad * gain
        mean_term = jnp.mean(scaled * normed, axis=-1, keepdims=True)
        result = res_ref[rows, :].astype(F32) + inv * (scaled - normed * mean_term)
        if as_rows:
            for lane in range(SUBL):
                outs[0][pl.ds(s * SUBL + lane, sub, stride=SUBL), :] = result[:, lane * LANES:(lane + 1) * LANES]
        else:
            outs[0][rows, :] = result
            outs[1][rows, :] = result.astype(BF16)
    dgain_ref[0:1, :] += total


def norm_grad(g, w, x, residual, gain, as_rows):
    tokens, width = g.shape
    dim = w.shape[0]
    tile, sub = 512, 256
    row = lambda w: pl.BlockSpec((tile, w), lambda m: (m, 0))
    one = lambda r, w: pl.BlockSpec((r, w), lambda m: (0, 0))
    if as_rows:
        out_specs = [pl.BlockSpec((tile * SUBL, LANES), lambda m: (m, 0))]
        out_shape = [jax.ShapeDtypeStruct((tokens * SUBL, LANES), F32)]
    else:
        out_specs = [row(dim), row(dim)]
        out_shape = [jax.ShapeDtypeStruct((tokens, dim), F32), jax.ShapeDtypeStruct((tokens, dim), BF16)]
    return pl.pallas_call(
        functools.partial(norm_grad_body, as_rows, sub),
        grid=(tokens // tile,),
        in_specs=[row(width), pl.BlockSpec((dim, width), lambda m: (0, 0), pipeline_mode=pl.Buffered(1)), row(dim), row(dim), one(1, dim)],
        out_specs=out_specs + [one(SUBL, dim)],
        out_shape=out_shape + [jax.ShapeDtypeStruct((SUBL, dim), F32)],
        compiler_params=pltpu.CompilerParams(dimension_semantics=("arbitrary",), vmem_limit_bytes=VMEM_LIMIT),
        cost_estimate=pl.CostEstimate(flops=2 * tokens * dim * width, bytes_accessed=2 * tokens * width + 2 * dim * width + 12 * tokens * dim, transcendentals=0),
    )(g, w, x, residual, gain)


def norm_fwd(values):
    values_f = values.astype(F32)
    inv_rms = lax.rsqrt(jnp.mean(values_f * values_f, axis=-1, keepdims=True) + NORM_EPS)
    return values_f * inv_rms, inv_rms


def gather_rows(shard):
    return lax.all_gather(shard, AXIS_NAME, tiled=True)


def scatter_rows(grad):
    return lax.psum_scatter(grad, AXIS_NAME, scatter_dimension=0, tiled=True)


def partner_sum(keep, send):
    n_dev = lax.axis_size(AXIS_NAME)
    return keep + lax.ppermute(send, AXIS_NAME, [(i, i ^ 1) for i in range(n_dev)])


def scatter_rows_by_chip(value):
    n_dev = lax.axis_size(AXIS_NAME)
    groups = [list(range(core, n_dev, 2)) for core in range(2)]
    return lax.psum_scatter(value, AXIS_NAME, scatter_dimension=0, tiled=True, axis_index_groups=groups)


def pick_block(value, index, dim):
    return lax.dynamic_index_in_dim(value, index, dim, keepdims=False)


def side_by_side(gate, up):
    rows, ff = gate.shape
    tiles = ff // FF_TILE
    both = jnp.stack([gate.reshape(rows, tiles, FF_TILE), up.reshape(rows, tiles, FF_TILE)], axis=2)
    return both.reshape(rows, 2 * ff)


def take_apart(both):
    rows, width = both.shape
    parts = both.reshape(rows, width // (2 * FF_TILE), 2, FF_TILE)
    return parts[:, :, 0].reshape(rows, width // 2), parts[:, :, 1].reshape(rows, width // 2)


def solution(mesh):
    row_spec = P(AXIS_NAME, None)
    vec_spec = P(AXIS_NAME)
    full_spec = P(None)
    batch_spec = P(AXIS_NAME, None, None)
    weight_specs = (vec_spec, row_spec, row_spec, row_spec, full_spec, full_spec, row_spec, vec_spec, row_spec, row_spec, row_spec)

    def device_step(tokens, positions, table, attn_norm, w_query, w_key, w_value, q_norm, k_norm, w_out, mlp_norm, w_gate, w_up, w_down, dy_out):
        n_seq, seq = tokens.shape
        n_tok = n_seq * seq
        rows_local, dim = table.shape
        head = q_norm.shape[0]
        kv_heads = w_key.shape[1] // head
        rep = w_query.shape[1] // w_key.shape[1]
        q_width, kv_width = w_query.shape[1], w_key.shape[1]

        all_ids = gather_rows(tokens.reshape(-1))
        n_dev = all_ids.shape[0] // n_tok
        local_ids = all_ids - lax.axis_index(AXIS_NAME) * rows_local
        is_owner = (local_ids >= 0) & (local_ids < rows_local)
        owned_ids = jnp.where(is_owner, local_ids, rows_local)

        w_qkv = gather_rows(jnp.concatenate([w_query, w_key, w_value], axis=1))
        out_half = w_out.shape[0] // 2
        gain_cols = jnp.pad(jnp.stack([attn_norm, mlp_norm], axis=1), ((0, 0), (0, LANES - 2)))
        w_o = gather_rows(jnp.concatenate([w_out[:out_half], w_out[out_half:], gain_cols], axis=1))
        n_lead = 5 * n_seq // 8
        lead_tok = n_lead * seq
        core = lax.axis_index(AXIS_NAME) & 1
        n_chip = n_dev // 2
        by_dev = owned_ids.reshape(n_chip, 2, n_tok)
        keep_ids, send_ids = pick_block(by_dev, core, 1), pick_block(by_dev, 1 - core, 1)
        parts = [send_ids[:, :lead_tok], keep_ids[:, :lead_tok], send_ids[:, lead_tok:], keep_ids[:, lead_tok:]]
        send_a, keep_a, send_b, keep_b = table_gather(table, jnp.concatenate([p.reshape(-1) for p in parts]), [p.size for p in parts])
        sum_a = partner_sum(keep_a, send_a)
        x_a = scatter_rows_by_chip(sum_a).reshape(lead_tok, dim)
        sum_b = partner_sum(keep_b, send_b)
        x_b = scatter_rows_by_chip(sum_b).reshape(n_tok - lead_tok, dim)

        gu_local, down_local, _ = lax.optimization_barrier((side_by_side(w_gate, w_up), w_down, keep_b))
        w_gu = gather_rows(gu_local)
        w_d = gather_rows(down_local)
        gains = w_o[:, 2 * dim:2 * dim + 2].astype(F32).T
        attn_gain, mlp_gain = gains[0:1], gains[1:2]

        sid, perm = lax.sort([owned_ids, lax.iota(jnp.int32, all_ids.shape[0])], num_keys=1, is_stable=False)
        out_rows = block_of(rows_local, 300, SUBL)
        edges = lax.iota(jnp.int32, rows_local // out_rows + 1) * out_rows
        bst = jnp.sum((owned_ids[None, :] < edges[:, None]).astype(jnp.int32), axis=1)

        half = head // 2
        inv_freq = jnp.exp(jnp.arange(half, dtype=F32) * (-2.0 * math.log(ROPE_THETA) / head))
        angles = positions.reshape(-1).astype(F32)[:, None] * inv_freq
        cos_h, sin_h = jnp.cos(angles), jnp.sin(angles)
        cos_t = jnp.concatenate([cos_h, cos_h], axis=1)
        sin_t = jnp.concatenate([-sin_h, sin_h], axis=1)
        q_gain = q_norm.astype(F32)[None]
        k_gain = k_norm.astype(F32)[None]

        w_o = jnp.concatenate([w_o[:, :dim], w_o[:, dim:2 * dim]], axis=0)

        def attn_norm_of(x_part):
            normed, _ = norm_fwd(x_part)
            return (normed * attn_gain).astype(BF16)

        qkv_a = dot_nn(attn_norm_of(x_a), w_qkv).astype(BF16)
        heads = attn_fwd(qkv_a, cos_t, sin_t, q_gain, k_gain, n_seq, seq, kv_heads, rep, 0, None)
        qkv_b = dot_nn(attn_norm_of(x_b), w_qkv).astype(BF16)
        heads = attn_fwd(qkv_b, cos_t, sin_t, q_gain, k_gain, n_seq, seq, kv_heads, rep, n_lead, heads)
        x_a, x_b, heads = lax.optimization_barrier((x_a, x_b, heads))
        x_emb = jnp.concatenate([x_a, x_b])
        hidden = (x_emb.astype(F32) + dot_nn(heads, w_o)).astype(BF16)
        normed2, _ = norm_fwd(hidden)
        mlp_in = (normed2 * mlp_gain).astype(BF16)
        gu, act = swiglu_fwd(mlp_in, w_gu)
        dy = dy_out.reshape(n_tok, dim)

        down_full, dy_later = lax.optimization_barrier((dot_tn(act, dy), dy))
        d_down = scatter_rows(down_full)
        dgu = swiglu_bwd(dy_later, w_d, gu)
        gu_full, dgu = lax.optimization_barrier((dot_tn(mlp_in, dgu), dgu))
        d_gu = scatter_rows(gu_full)
        grad_hidden, hidden_b, d_mlp_norm = norm_grad(dgu, w_gu, hidden, dy, mlp_gain, False)
        grad_heads = dot_nt(hidden_b, w_o).astype(BF16)
        dqkv, dqn, dkn = attn_bwd(qkv_a, qkv_b, grad_heads, cos_t, sin_t, q_gain, k_gain, seq, kv_heads, rep)
        grad_x, d_attn_norm = norm_grad(dqkv, w_qkv, x_emb, grad_hidden, attn_gain, True)
        grad_x = grad_x.reshape(n_tok, SUBL, LANES)
        grad_x, dqkv, act_later, hidden_later, x_later = lax.optimization_barrier((grad_x, dqkv, act, hidden_b, x_emb))
        all_rows = gather_rows(grad_x)
        d_out_full = dot_tn(heads, hidden_later)
        mid = d_out_full.shape[0] // 2
        qkvo_full = jnp.concatenate([dot_tn(attn_norm_of(x_later), dqkv), d_out_full[:mid], d_out_full[mid:]], axis=1)
        qkvo_full = qkvo_full.reshape(n_chip, 2, -1, qkvo_full.shape[1])
        qkvo_sum = partner_sum(pick_block(qkvo_full, core, 1), pick_block(qkvo_full, 1 - core, 1))
        d_qkvo = scatter_rows_by_chip(qkvo_sum.reshape(-1, qkvo_sum.shape[-1]))
        layer_out = (hidden.astype(F32) + dot_nn(act_later, w_d)).astype(BF16)

        small = lax.psum(jnp.concatenate([d_attn_norm[0], d_mlp_norm[0], dqn[0], dkn[0]]), AXIS_NAME)
        shard_len = attn_norm.shape[0]
        at = lax.axis_index(AXIS_NAME) * shard_len
        d_attn_norm = lax.dynamic_slice(small, (at,), (shard_len,))
        d_mlp_norm = lax.dynamic_slice(small, (dim + at,), (shard_len,))
        d_q_norm = small[2 * dim:2 * dim + head]
        d_k_norm = small[2 * dim + head:]

        d_table = table_scatter(all_rows, perm, sid, bst, rows_local, out_rows)
        d_gate, d_up = take_apart(d_gu)
        cuts = [q_width, q_width + kv_width, q_width + 2 * kv_width, q_width + 2 * kv_width + dim]
        d_query, d_key, d_value, out_even, out_odd = jnp.split(d_qkvo, cuts, axis=1)
        d_out = jnp.concatenate([out_even, out_odd], axis=0)
        return (layer_out.reshape(n_seq, seq, dim), d_table, d_attn_norm, d_query, d_key, d_value, d_q_norm, d_k_norm, d_out, d_mlp_norm, d_gate, d_up, d_down)

    return jax.shard_map(device_step, mesh=mesh, in_specs=(row_spec, row_spec, row_spec) + weight_specs + (batch_spec,), out_specs=(batch_spec, row_spec) + weight_specs, check_vma=False)
```

```python
import functools
import math
import jax
import jax.numpy as jnp
from jax import lax
from jax.experimental import pallas as pl
from jax.experimental.pallas import tpu as pltpu
from jax.sharding import PartitionSpec as P

NORM_EPS = 1e-6
ROPE_THETA = 1.0e6
AXIS_NAME = 'fsdp'
F32 = jnp.float32
BF16 = jnp.bfloat16
LANES = 128
SUBL = 8
VMEM_LIMIT = 60 * 1024 * 1024


def dot_nt(a, b):
    return lax.dot_general(a, b, (((1,), (1,)), ((), ())), preferred_element_type=F32)


def dot_tn(a, b):
    return lax.dot_general(a, b, (((0,), (0,)), ((), ())), preferred_element_type=F32)


def dot_nn(a, b):
    return jnp.dot(a, b, preferred_element_type=F32)


def block_of(total, limit, step):
    best = step
    for size in range(step, limit + 1, step):
        if total % size == 0:
            best = size
    return best


def gather_body(n_tab, starts, tab_rows, tok_rows, idx_ref, tab_ref, *refs):
    out_refs, (store, stage) = refs[:-2], refs[-2:]
    step = pl.program_id(0)

    @pl.when(step == 0)
    def _():
        store[n_tab * tab_rows] = jnp.zeros((SUBL, LANES), BF16)

    @pl.when(step < n_tab)
    def _():
        for lane in range(SUBL):
            stage[pl.ds(lane, tab_rows, stride=SUBL + 1), :] = tab_ref[:, lane * LANES:(lane + 1) * LANES].astype(F32)

        def put(it, carry):
            for u in range(32):
                row = it * 32 + u
                store[step * tab_rows + row] = stage[pl.ds(row * (SUBL + 1), SUBL), :].astype(BF16)
            return carry

        lax.fori_loop(0, tab_rows // 32, put, 0)

    def copy_rows(out_ref):
        base = (step - n_tab) * tok_rows
        unroll = 32

        def loop(it, carry):
            first = it * unroll
            for u in range(unroll):
                out_ref[first + u] = store[idx_ref[base + first + u]]
            return carry

        lax.fori_loop(0, tok_rows // unroll, loop, 0)

    for k, out_ref in enumerate(out_refs):
        @pl.when((step >= n_tab + starts[k]) & (step < n_tab + starts[k + 1]))
        def _(out_ref=out_ref):
            copy_rows(out_ref)


def table_gather(table, idx, counts):
    rows, width = table.shape
    tab_rows = block_of(rows, 640, 32)
    n_tab = rows // tab_rows
    tok_rows = 512
    starts = [sum(counts[:k]) // tok_rows for k in range(len(counts) + 1)]
    out_spec = lambda lo, hi: pl.BlockSpec((tok_rows, SUBL, LANES), lambda s, ids: (jnp.clip(s - n_tab - lo, 0, hi - lo - 1), 0, 0))
    grid_spec = pltpu.PrefetchScalarGridSpec(
        num_scalar_prefetch=1,
        grid=(n_tab + starts[-1],),
        in_specs=[pl.BlockSpec((tab_rows, width), lambda s, ids: (jnp.minimum(s, n_tab - 1), 0))],
        out_specs=[out_spec(lo, hi) for lo, hi in zip(starts, starts[1:])],
        scratch_shapes=[pltpu.VMEM((rows + 8, SUBL, LANES), BF16), pltpu.VMEM((tab_rows * (SUBL + 1), LANES), F32)],
    )
    return pl.pallas_call(
        functools.partial(gather_body, n_tab, starts, tab_rows, tok_rows),
        grid_spec=grid_spec,
        out_shape=[jax.ShapeDtypeStruct((n, SUBL, LANES), BF16) for n in counts],
        compiler_params=pltpu.CompilerParams(dimension_semantics=("arbitrary",), vmem_limit_bytes=VMEM_LIMIT),
        cost_estimate=pl.CostEstimate(flops=70_000_000_000, bytes_accessed=rows * width * 2 + sum(counts) * width * 2, transcendentals=0),
        name="table_gather",
    )(idx, table)


def scatter_body(group, slots, out_rows, perm_ref, sid_ref, bst_ref, rows_ref, out_ref, acc, ring, sem):
    blk = pl.program_id(0)
    total = bst_ref[pl.num_programs(0)]
    n_groups = (total + group - 1) // group

    def issue(g):
        slot = lax.rem(g, slots)
        for u in range(group):
            pltpu.make_async_copy(rows_ref.at[perm_ref[g * group + u]], ring.at[slot * group + u], sem.at[slot]).start()

    @pl.when(blk == 0)
    def _():
        def first(g, carry):
            issue(g)
            return carry

        lax.fori_loop(0, jnp.minimum(n_groups, slots), first, 0)

    acc[...] = jnp.zeros(acc.shape, F32)
    low = bst_ref[blk]
    high = bst_ref[blk + 1]
    g_first = low // group
    g_last = jnp.where(high > low, (high + group - 1) // group, g_first)
    base = blk * out_rows

    def per_group(g, carry):
        start = g * group
        slot = lax.rem(g, slots)

        @pl.when(start >= low)
        def _():
            pltpu.make_async_copy(rows_ref.at[pl.ds(0, group)], ring.at[pl.ds(slot * group, group)], sem.at[slot]).wait()

        prev, prev_id = carry
        for u in range(group):
            row_id = sid_ref[start + u]
            local = row_id - base
            inside = (local >= 0) & (local < out_rows)
            value = ring[slot * group + u]
            value = jnp.where(row_id == prev_id, prev + value, value)
            acc[pl.ds(pl.multiple_of(jnp.where(inside, local, out_rows) * SUBL, SUBL), SUBL), :] = value
            prev, prev_id = value, row_id

        @pl.when((high >= start + group) & (g + slots < n_groups))
        def _():
            issue(g + slots)

        return prev, prev_id

    lax.fori_loop(g_first, g_last, per_group, (jnp.zeros((SUBL, LANES), F32), jnp.int32(-1)))
    for lane in range(SUBL):
        out_ref[:, lane * LANES:(lane + 1) * LANES] = acc[pl.ds(lane, out_rows, stride=SUBL), :]


def table_scatter(rows, perm, sid, bst, n_rows, out_rows):
    total = rows.shape[0]
    width = SUBL * LANES
    group, slots = 16, 16
    grid_spec = pltpu.PrefetchScalarGridSpec(
        num_scalar_prefetch=3,
        grid=(n_rows // out_rows,),
        in_specs=[pl.BlockSpec(memory_space=pl.ANY)],
        out_specs=pl.BlockSpec((out_rows, width), lambda b, *_: (b, 0)),
        scratch_shapes=[pltpu.VMEM((out_rows * SUBL + SUBL, LANES), F32), pltpu.VMEM((group * slots, SUBL, LANES), F32), pltpu.SemaphoreType.DMA((slots,))],
    )
    return pl.pallas_call(
        functools.partial(scatter_body, group, slots, out_rows),
        grid_spec=grid_spec,
        out_shape=jax.ShapeDtypeStruct((n_rows, width), F32),
        compiler_params=pltpu.CompilerParams(dimension_semantics=("arbitrary",), vmem_limit_bytes=32 * 1024 * 1024),
        cost_estimate=pl.CostEstimate(flops=70_000_000_000, bytes_accessed=n_rows * width * 4 + total * width * 4, transcendentals=0),
        name="table_scatter",
    )(perm, sid, bst, rows)


def head_prep(raw, gain, cos_t, sin_t):
    values = raw.astype(F32)
    inv = lax.rsqrt(jnp.mean(values * values, axis=-1, keepdims=True) + NORM_EPS)
    normed = values * inv
    scaled = normed * gain
    rot = scaled * cos_t + pltpu.roll(scaled, LANES // 2, 1) * sin_t
    return rot.astype(BF16), normed, inv


def head_prep_bwd(grad, normed, inv, gain, cos_t, sin_t):
    grad_t = grad * cos_t - pltpu.roll(grad, LANES // 2, 1) * sin_t
    grad_gain = jnp.sum(grad_t * normed, axis=0, keepdims=True)
    grad_n = grad_t * gain
    mean_term = jnp.mean(grad_n * normed, axis=-1, keepdims=True)
    return (inv * (grad_n - normed * mean_term)).astype(BF16), grad_gain


def exp_scaled(scores, peak):
    return jnp.exp2((scores - peak) * (LANES ** -0.5 * math.log2(math.e)))


def probs_by_key(q_rot, k_rot, tri):
    h = tri.shape[0]
    top = dot_nt(k_rot[:h], q_rot)
    s_ll = jnp.where(tri, top[:, :h], -1e30)
    s_lh = top[:, h:]
    s_hh = jnp.where(tri, dot_nt(k_rot[h:], q_rot[h:]), -1e30)
    peak_l = jnp.max(s_ll, axis=0, keepdims=True)
    peak_h = jnp.maximum(jnp.max(s_lh, axis=0, keepdims=True), jnp.max(s_hh, axis=0, keepdims=True))
    e_ll, e_lh, e_hh = exp_scaled(s_ll, peak_l), exp_scaled(s_lh, peak_h), exp_scaled(s_hh, peak_h)
    r_l = 1.0 / jnp.sum(e_ll, axis=0, keepdims=True)
    r_h = 1.0 / (jnp.sum(e_lh, axis=0, keepdims=True) + jnp.sum(e_hh, axis=0, keepdims=True))
    return e_ll * r_l, e_lh * r_h, e_hh * r_h


def causal_by_key(seq):
    h = seq // 2
    return lax.broadcasted_iota(jnp.int32, (h, h), 0) <= lax.broadcasted_iota(jnp.int32, (h, h), 1)


def col(start, width):
    return pl.ds(pl.multiple_of(start, LANES), width)


KV_UNROLL = 4


def attn_fwd_body(kv_heads, rep, aliased, *refs):
    if aliased:
        refs = refs[:5] + refs[6:]
    qkv_ref, cos_ref, sin_ref, qn_ref, kn_ref, out_ref = refs
    cos_t, sin_t = cos_ref[...], sin_ref[...]
    q_gain, k_gain = qn_ref[...], kn_ref[...]
    tri = causal_by_key(qkv_ref.shape[0])
    h = tri.shape[0]
    k_base = kv_heads * rep * LANES
    v_base = k_base + kv_heads * LANES

    def per_kv(it, carry):
        for step in range(KV_UNROLL):
            g = it * KV_UNROLL + step
            k_rot, _, _ = head_prep(qkv_ref[:, col(k_base + g * LANES, LANES)], k_gain, cos_t, sin_t)
            v_raw = qkv_ref[:, col(v_base + g * LANES, LANES)]
            for r in range(rep):
                q_rot, _, _ = head_prep(qkv_ref[:, col((g * rep + r) * LANES, LANES)], q_gain, cos_t, sin_t)
                p_ll, p_lh, p_hh = [p.astype(BF16) for p in probs_by_key(q_rot, k_rot, tri)]
                at = col((r * kv_heads + g) * LANES, LANES)
                out_ref[:h, at] = dot_tn(p_ll, v_raw[:h]).astype(BF16)
                out_ref[h:, at] = dot_tn(jnp.concatenate([p_lh, p_hh], axis=0), v_raw).astype(BF16)
        return carry

    lax.fori_loop(0, kv_heads // KV_UNROLL, per_kv, 0)


def attn_bwd_body(kv_heads, rep, n_lead, lead_ref, tail_ref, do_ref, cos_ref, sin_ref, qn_ref, kn_ref, dqkv_ref, dqn_ref, dkn_ref):
    cos_t, sin_t = cos_ref[...], sin_ref[...]
    q_gain, k_gain = qn_ref[...], kn_ref[...]
    tri = causal_by_key(do_ref.shape[0])
    h = tri.shape[0]
    k_base = kv_heads * rep * LANES
    v_base = k_base + kv_heads * LANES
    scale = LANES ** -0.5

    @pl.when(pl.program_id(0) == 0)
    def _():
        dqn_ref[...] = jnp.zeros(dqn_ref.shape, F32)
        dkn_ref[...] = jnp.zeros(dkn_ref.shape, F32)

    def one_seq(qkv_ref):
        def one_kv(g, dqn, dkn):
            k_at = col(k_base + g * LANES, LANES)
            v_at = col(v_base + g * LANES, LANES)
            k_rot, k_normed, k_inv = head_prep(qkv_ref[:, k_at], k_gain, cos_t, sin_t)
            v_raw = qkv_ref[:, v_at]
            dk_l, dk_h, dv_l, dv_h = [], [], [], []
            for r in range(rep):
                at = col((g * rep + r) * LANES, LANES)
                q_rot, q_normed, q_inv = head_prep(qkv_ref[:, at], q_gain, cos_t, sin_t)
                grad_o = do_ref[:, col((r * kv_heads + g) * LANES, LANES)]
                p_ll, p_lh, p_hh = probs_by_key(q_rot, k_rot, tri)
                g_top = dot_nt(v_raw[:h], grad_o)
                g_ll, g_lh = g_top[:, :h], g_top[:, h:]
                g_hh = dot_nt(v_raw[h:], grad_o[h:])
                t_l = jnp.sum(g_ll * p_ll, axis=0, keepdims=True)
                t_h = jnp.sum(g_lh * p_lh, axis=0, keepdims=True) + jnp.sum(g_hh * p_hh, axis=0, keepdims=True)
                s_ll = (p_ll * ((g_ll - t_l) * scale)).astype(BF16)
                s_lh = (p_lh * ((g_lh - t_h) * scale)).astype(BF16)
                s_hh = (p_hh * ((g_hh - t_h) * scale)).astype(BF16)
                dv_l.append(dot_nn(jnp.concatenate([p_ll.astype(BF16), p_lh.astype(BF16)], axis=1), grad_o))
                dv_h.append(dot_nn(p_hh.astype(BF16), grad_o[h:]))
                dk_l.append(dot_nn(jnp.concatenate([s_ll, s_lh], axis=1), q_rot))
                dk_h.append(dot_nn(s_hh, q_rot[h:]))
                dq = jnp.concatenate([dot_tn(s_ll, k_rot[:h]), dot_tn(jnp.concatenate([s_lh, s_hh], axis=0), k_rot)], axis=0)
                dq_raw, gain_part = head_prep_bwd(dq, q_normed, q_inv, q_gain, cos_t, sin_t)
                dqn = dqn + gain_part
                dqkv_ref[:, at] = dq_raw
            dk = jnp.concatenate([sum(dk_l[1:], dk_l[0]), sum(dk_h[1:], dk_h[0])], axis=0)
            dk_raw, gain_part = head_prep_bwd(dk, k_normed, k_inv, k_gain, cos_t, sin_t)
            dkn = dkn + gain_part
            dqkv_ref[:, k_at] = dk_raw
            dqkv_ref[:h, v_at] = sum(dv_l[1:], dv_l[0]).astype(BF16)
            dqkv_ref[h:, v_at] = sum(dv_h[1:], dv_h[0]).astype(BF16)
            return dqn, dkn

        def per_kv(it, carry):
            for step in range(KV_UNROLL):
                carry = one_kv(it * KV_UNROLL + step, *carry)
            return carry

        zero = jnp.zeros((1, LANES), F32)
        dqn, dkn = lax.fori_loop(0, kv_heads // KV_UNROLL, per_kv, (zero, zero))
        dqn_ref[0:1, :] += dqn
        dkn_ref[0:1, :] += dkn

    @pl.when(pl.program_id(0) < n_lead)
    def _():
        one_seq(lead_ref)

    @pl.when(pl.program_id(0) >= n_lead)
    def _():
        one_seq(tail_ref)


def attn_fwd(qkv, cos_t, sin_t, q_gain, k_gain, n_seq, seq, kv_heads, rep, first, into):
    tokens, width = qkv.shape
    q_width = kv_heads * rep * LANES
    own = lambda w: pl.BlockSpec((seq, w), lambda b: (b, 0))
    shifted = lambda w: pl.BlockSpec((seq, w), lambda b: (b + first, 0))
    one = lambda r, w: pl.BlockSpec((r, w), lambda b: (0, 0))
    in_specs = [own(width), shifted(LANES), shifted(LANES), one(1, LANES), one(1, LANES)]
    args = (qkv, cos_t, sin_t, q_gain, k_gain)
    aliases = {}
    if into is not None:
        in_specs.append(pl.BlockSpec(memory_space=pl.ANY))
        args += (into,)
        aliases = {5: 0}
    return pl.pallas_call(
        functools.partial(attn_fwd_body, kv_heads, rep, into is not None),
        grid=(tokens // seq,),
        in_specs=in_specs,
        out_specs=shifted(q_width),
        out_shape=jax.ShapeDtypeStruct((n_seq * seq, q_width), BF16),
        input_output_aliases=aliases,
        compiler_params=pltpu.CompilerParams(dimension_semantics=("arbitrary",), vmem_limit_bytes=32 * 1024 * 1024),
        cost_estimate=pl.CostEstimate(flops=25_000_000_000, bytes_accessed=tokens * (width + q_width) * 2, transcendentals=4_200_000),
        name="attn_fwd",
    )(*args)


def attn_bwd(lead, tail, grad_o, cos_t, sin_t, q_gain, k_gain, seq, kv_heads, rep):
    tokens, q_width = grad_o.shape
    width = lead.shape[1]
    n_lead = lead.shape[0] // seq
    row = lambda w: pl.BlockSpec((seq, w), lambda b: (b, 0))
    one = lambda r, w: pl.BlockSpec((r, w), lambda b: (0, 0))
    lead_spec = pl.BlockSpec((seq, width), lambda b: (jnp.minimum(b, n_lead - 1), 0))
    tail_spec = pl.BlockSpec((seq, width), lambda b: (jnp.maximum(b - n_lead, 0), 0))
    return pl.pallas_call(
        functools.partial(attn_bwd_body, kv_heads, rep, n_lead),
        grid=(tokens // seq,),
        in_specs=[lead_spec, tail_spec, row(q_width), row(LANES), row(LANES), one(1, LANES), one(1, LANES)],
        out_specs=[row(width), one(SUBL, LANES), one(SUBL, LANES)],
        out_shape=[jax.ShapeDtypeStruct((tokens, width), BF16), jax.ShapeDtypeStruct((SUBL, LANES), F32), jax.ShapeDtypeStruct((SUBL, LANES), F32)],
        compiler_params=pltpu.CompilerParams(dimension_semantics=("arbitrary",), vmem_limit_bytes=40 * 1024 * 1024),
        cost_estimate=pl.CostEstimate(flops=100_000_000_000, bytes_accessed=tokens * (2 * width + q_width) * 2, transcendentals=8_400_000),
        name="attn_bwd",
    )(lead, tail, grad_o, cos_t, sin_t, q_gain, k_gain)


FF_TILE = 512
ROW_TILE = 1024
SUB_ROWS = 256


def swiglu_fwd_body(x_ref, w_ref, gu_ref, act_ref):
    for s in range(0, x_ref.shape[0], SUB_ROWS):
        rows = slice(s, s + SUB_ROWS)
        both = dot_nn(x_ref[rows, :], w_ref[...])
        gu_ref[rows, :] = both
        gate, up = both[:, :FF_TILE], both[:, FF_TILE:]
        act_ref[rows, :] = (gate * jax.nn.sigmoid(gate) * up).astype(BF16)


def swiglu_fwd(x, w_gu):
    tokens, dim = x.shape
    both = w_gu.shape[1]
    ff = both // 2
    return pl.pallas_call(
        swiglu_fwd_body,
        grid=(ff // FF_TILE, tokens // ROW_TILE),
        in_specs=[pl.BlockSpec((ROW_TILE, dim), lambda n, m: (m, 0)), pl.BlockSpec((dim, 2 * FF_TILE), lambda n, m: (0, n))],
        out_specs=[pl.BlockSpec((ROW_TILE, 2 * FF_TILE), lambda n, m: (m, n)), pl.BlockSpec((ROW_TILE, FF_TILE), lambda n, m: (m, n))],
        out_shape=[jax.ShapeDtypeStruct((tokens, both), F32), jax.ShapeDtypeStruct((tokens, ff), BF16)],
        compiler_params=pltpu.CompilerParams(dimension_semantics=("arbitrary", "arbitrary"), vmem_limit_bytes=40 * 1024 * 1024),
        cost_estimate=pl.CostEstimate(flops=2 * tokens * dim * both, bytes_accessed=tokens * both * 5, transcendentals=tokens * ff),
        name="swiglu_fwd",
    )(x, w_gu)


def swiglu_bwd_body(dy_ref, w_ref, gu_ref, dgu_ref):
    for s in range(0, dy_ref.shape[0], SUB_ROWS):
        rows = slice(s, s + SUB_ROWS)
        grad_act = dot_nt(dy_ref[rows, :], w_ref[...])
        gate, up = gu_ref[rows, :FF_TILE], gu_ref[rows, FF_TILE:]
        sig = jax.nn.sigmoid(gate)
        part = grad_act * sig
        dgu_ref[rows, :FF_TILE] = (part * up * (1.0 + gate * (1.0 - sig))).astype(BF16)
        dgu_ref[rows, FF_TILE:] = (part * gate).astype(BF16)


def swiglu_bwd(dy, w_down, gu):
    tokens, dim = dy.shape
    ff = w_down.shape[0]
    return pl.pallas_call(
        swiglu_bwd_body,
        grid=(ff // FF_TILE, tokens // ROW_TILE),
        in_specs=[pl.BlockSpec((ROW_TILE, dim), lambda n, m: (m, 0)), pl.BlockSpec((FF_TILE, dim), lambda n, m: (n, 0)), pl.BlockSpec((ROW_TILE, 2 * FF_TILE), lambda n, m: (m, n))],
        out_specs=pl.BlockSpec((ROW_TILE, 2 * FF_TILE), lambda n, m: (m, n)),
        out_shape=jax.ShapeDtypeStruct((tokens, 2 * ff), BF16),
        compiler_params=pltpu.CompilerParams(dimension_semantics=("arbitrary", "arbitrary"), vmem_limit_bytes=40 * 1024 * 1024),
        cost_estimate=pl.CostEstimate(flops=2 * tokens * dim * ff, bytes_accessed=tokens * ff * 12, transcendentals=tokens * ff),
        name="swiglu_bwd",
    )(dy, w_down, gu)


def norm_grad_body(as_rows, sub, g_ref, w_ref, x_ref, res_ref, gain_ref, *outs):
    gain = gain_ref[...]
    dgain_ref = outs[-1]

    @pl.when(pl.program_id(0) == 0)
    def _():
        dgain_ref[...] = jnp.zeros(dgain_ref.shape, F32)

    total = jnp.zeros(gain.shape, F32)
    for s in range(0, g_ref.shape[0], sub):
        rows = slice(s, s + sub)
        grad = dot_nt(g_ref[rows, :], w_ref[...])
        values = x_ref[rows, :].astype(F32)
        inv = lax.rsqrt(jnp.mean(values * values, axis=-1, keepdims=True) + NORM_EPS)
        normed = values * inv
        total = total + jnp.sum(grad * normed, axis=0, keepdims=True)
        scaled = grad * gain
        mean_term = jnp.mean(scaled * normed, axis=-1, keepdims=True)
        result = res_ref[rows, :].astype(F32) + inv * (scaled - normed * mean_term)
        if as_rows:
            for lane in range(SUBL):
                outs[0][pl.ds(s * SUBL + lane, sub, stride=SUBL), :] = result[:, lane * LANES:(lane + 1) * LANES]
        else:
            outs[0][rows, :] = result
            outs[1][rows, :] = result.astype(BF16)
    dgain_ref[0:1, :] += total


def norm_grad(g, w, x, residual, gain, as_rows):
    tokens, width = g.shape
    dim = w.shape[0]
    tile, sub = 512, 256
    row = lambda w: pl.BlockSpec((tile, w), lambda m: (m, 0))
    one = lambda r, w: pl.BlockSpec((r, w), lambda m: (0, 0))
    if as_rows:
        out_specs = [pl.BlockSpec((tile * SUBL, LANES), lambda m: (m, 0))]
        out_shape = [jax.ShapeDtypeStruct((tokens * SUBL, LANES), F32)]
    else:
        out_specs = [row(dim), row(dim)]
        out_shape = [jax.ShapeDtypeStruct((tokens, dim), F32), jax.ShapeDtypeStruct((tokens, dim), BF16)]
    return pl.pallas_call(
        functools.partial(norm_grad_body, as_rows, sub),
        grid=(tokens // tile,),
        in_specs=[row(width), pl.BlockSpec((dim, width), lambda m: (0, 0), pipeline_mode=pl.Buffered(1)), row(dim), row(dim), one(1, dim)],
        out_specs=out_specs + [one(SUBL, dim)],
        out_shape=out_shape + [jax.ShapeDtypeStruct((SUBL, dim), F32)],
        compiler_params=pltpu.CompilerParams(dimension_semantics=("arbitrary",), vmem_limit_bytes=VMEM_LIMIT),
        cost_estimate=pl.CostEstimate(flops=2 * tokens * dim * width, bytes_accessed=2 * tokens * width + 2 * dim * width + 12 * tokens * dim, transcendentals=0),
    )(g, w, x, residual, gain)


def norm_fwd(values):
    values_f = values.astype(F32)
    inv_rms = lax.rsqrt(jnp.mean(values_f * values_f, axis=-1, keepdims=True) + NORM_EPS)
    return values_f * inv_rms, inv_rms


def gather_rows(shard):
    return lax.all_gather(shard, AXIS_NAME, tiled=True)


def scatter_rows(grad):
    return lax.psum_scatter(grad, AXIS_NAME, scatter_dimension=0, tiled=True)


def partner_sum(keep, send):
    n_dev = lax.axis_size(AXIS_NAME)
    return keep + lax.ppermute(send, AXIS_NAME, [(i, i ^ 1) for i in range(n_dev)])


def scatter_rows_by_chip(value):
    n_dev = lax.axis_size(AXIS_NAME)
    groups = [list(range(core, n_dev, 2)) for core in range(2)]
    return lax.psum_scatter(value, AXIS_NAME, scatter_dimension=0, tiled=True, axis_index_groups=groups)


def pick_block(value, index, dim):
    return lax.dynamic_index_in_dim(value, index, dim, keepdims=False)


def side_by_side(gate, up):
    rows, ff = gate.shape
    tiles = ff // FF_TILE
    both = jnp.stack([gate.reshape(rows, tiles, FF_TILE), up.reshape(rows, tiles, FF_TILE)], axis=2)
    return both.reshape(rows, 2 * ff)


def take_apart(both):
    rows, width = both.shape
    parts = both.reshape(rows, width // (2 * FF_TILE), 2, FF_TILE)
    return parts[:, :, 0].reshape(rows, width // 2), parts[:, :, 1].reshape(rows, width // 2)


def solution(mesh):
    row_spec = P(AXIS_NAME, None)
    vec_spec = P(AXIS_NAME)
    full_spec = P(None)
    batch_spec = P(AXIS_NAME, None, None)
    weight_specs = (vec_spec, row_spec, row_spec, row_spec, full_spec, full_spec, row_spec, vec_spec, row_spec, row_spec, row_spec)

    def device_step(tokens, positions, table, attn_norm, w_query, w_key, w_value, q_norm, k_norm, w_out, mlp_norm, w_gate, w_up, w_down, dy_out):
        n_seq, seq = tokens.shape
        n_tok = n_seq * seq
        rows_local, dim = table.shape
        head = q_norm.shape[0]
        kv_heads = w_key.shape[1] // head
        rep = w_query.shape[1] // w_key.shape[1]
        q_width, kv_width = w_query.shape[1], w_key.shape[1]

        all_ids = gather_rows(tokens.reshape(-1))
        n_dev = all_ids.shape[0] // n_tok
        local_ids = all_ids - lax.axis_index(AXIS_NAME) * rows_local
        is_owner = (local_ids >= 0) & (local_ids < rows_local)
        owned_ids = jnp.where(is_owner, local_ids, rows_local)

        w_qkv = gather_rows(jnp.concatenate([w_query, w_key, w_value], axis=1))
        out_half = w_out.shape[0] // 2
        gain_cols = jnp.pad(jnp.stack([attn_norm, mlp_norm], axis=1), ((0, 0), (0, LANES - 2)))
        w_o = gather_rows(jnp.concatenate([w_out[:out_half], w_out[out_half:], gain_cols], axis=1))
        n_lead = n_seq // 2
        lead_tok = n_lead * seq
        core = lax.axis_index(AXIS_NAME) & 1
        n_chip = n_dev // 2
        by_dev = owned_ids.reshape(n_chip, 2, n_tok)
        keep_ids, send_ids = pick_block(by_dev, core, 1), pick_block(by_dev, 1 - core, 1)
        parts = [send_ids[:, :lead_tok], keep_ids[:, :lead_tok], send_ids[:, lead_tok:], keep_ids[:, lead_tok:]]
        send_a, keep_a, send_b, keep_b = table_gather(table, jnp.concatenate([p.reshape(-1) for p in parts]), [p.size for p in parts])
        sum_a = partner_sum(keep_a, send_a)
        x_a = scatter_rows_by_chip(sum_a).reshape(lead_tok, dim)
        sum_b = partner_sum(keep_b, send_b)
        x_b = scatter_rows_by_chip(sum_b).reshape(n_tok - lead_tok, dim)

        gu_local, down_local, _ = lax.optimization_barrier((side_by_side(w_gate, w_up), w_down, keep_b))
        w_gu = gather_rows(gu_local)
        w_d = gather_rows(down_local)
        gains = w_o[:, 2 * dim:2 * dim + 2].astype(F32).T
        attn_gain, mlp_gain = gains[0:1], gains[1:2]

        sid, perm = lax.sort([owned_ids, lax.iota(jnp.int32, all_ids.shape[0])], num_keys=1, is_stable=False)
        out_rows = block_of(rows_local, 300, SUBL)
        edges = lax.iota(jnp.int32, rows_local // out_rows + 1) * out_rows
        bst = jnp.sum((owned_ids[None, :] < edges[:, None]).astype(jnp.int32), axis=1)

        half = head // 2
        inv_freq = jnp.exp(jnp.arange(half, dtype=F32) * (-2.0 * math.log(ROPE_THETA) / head))
        angles = positions.reshape(-1).astype(F32)[:, None] * inv_freq
        cos_h, sin_h = jnp.cos(angles), jnp.sin(angles)
        cos_t = jnp.concatenate([cos_h, cos_h], axis=1)
        sin_t = jnp.concatenate([-sin_h, sin_h], axis=1)
        q_gain = q_norm.astype(F32)[None]
        k_gain = k_norm.astype(F32)[None]

        w_o = jnp.concatenate([w_o[:, :dim], w_o[:, dim:2 * dim]], axis=0)

        def attn_norm_of(x_part):
            normed, _ = norm_fwd(x_part)
            return (normed * attn_gain).astype(BF16)

        qkv_a = dot_nn(attn_norm_of(x_a), w_qkv).astype(BF16)
        heads = attn_fwd(qkv_a, cos_t, sin_t, q_gain, k_gain, n_seq, seq, kv_heads, rep, 0, None)
        qkv_b = dot_nn(attn_norm_of(x_b), w_qkv).astype(BF16)
        heads = attn_fwd(qkv_b, cos_t, sin_t, q_gain, k_gain, n_seq, seq, kv_heads, rep, n_lead, heads)
        x_a, x_b, heads = lax.optimization_barrier((x_a, x_b, heads))
        x_emb = jnp.concatenate([x_a, x_b])
        hidden = (x_emb.astype(F32) + dot_nn(heads, w_o)).astype(BF16)
        normed2, _ = norm_fwd(hidden)
        mlp_in = (normed2 * mlp_gain).astype(BF16)
        gu, act = swiglu_fwd(mlp_in, w_gu)
        dy = dy_out.reshape(n_tok, dim)

        down_full, dy_later = lax.optimization_barrier((dot_tn(act, dy), dy))
        d_down = scatter_rows(down_full)
        dgu = swiglu_bwd(dy_later, w_d, gu)
        gu_full, dgu = lax.optimization_barrier((dot_tn(mlp_in, dgu), dgu))
        d_gu = scatter_rows(gu_full)
        grad_hidden, hidden_b, d_mlp_norm = norm_grad(dgu, w_gu, hidden, dy, mlp_gain, False)
        grad_heads = dot_nt(hidden_b, w_o).astype(BF16)
        dqkv, dqn, dkn = attn_bwd(qkv_a, qkv_b, grad_heads, cos_t, sin_t, q_gain, k_gain, seq, kv_heads, rep)
        grad_x, d_attn_norm = norm_grad(dqkv, w_qkv, x_emb, grad_hidden, attn_gain, True)
        grad_x = grad_x.reshape(n_tok, SUBL, LANES)
        grad_x, dqkv, act_later, hidden_later, x_later = lax.optimization_barrier((grad_x, dqkv, act, hidden_b, x_emb))
        all_rows = gather_rows(grad_x)
        d_out_full = dot_tn(heads, hidden_later)
        mid = d_out_full.shape[0] // 2
        qkvo_full = jnp.concatenate([dot_tn(attn_norm_of(x_later), dqkv), d_out_full[:mid], d_out_full[mid:]], axis=1)
        qkvo_full = qkvo_full.reshape(n_chip, 2, -1, qkvo_full.shape[1])
        qkvo_sum = partner_sum(pick_block(qkvo_full, core, 1), pick_block(qkvo_full, 1 - core, 1))
        d_qkvo = scatter_rows_by_chip(qkvo_sum.reshape(-1, qkvo_sum.shape[-1]))
        layer_out = (hidden.astype(F32) + dot_nn(act_later, w_d)).astype(BF16)

        small = lax.psum(jnp.concatenate([d_attn_norm[0], d_mlp_norm[0], dqn[0], dkn[0]]), AXIS_NAME)
        shard_len = attn_norm.shape[0]
        at = lax.axis_index(AXIS_NAME) * shard_len
        d_attn_norm = lax.dynamic_slice(small, (at,), (shard_len,))
        d_mlp_norm = lax.dynamic_slice(small, (dim + at,), (shard_len,))
        d_q_norm = small[2 * dim:2 * dim + head]
        d_k_norm = small[2 * dim + head:]

        d_table = table_scatter(all_rows, perm, sid, bst, rows_local, out_rows)
        d_gate, d_up = take_apart(d_gu)
        cuts = [q_width, q_width + kv_width, q_width + 2 * kv_width, q_width + 2 * kv_width + dim]
        d_query, d_key, d_value, out_even, out_odd = jnp.split(d_qkvo, cuts, axis=1)
        d_out = jnp.concatenate([out_even, out_odd], axis=0)
        return (layer_out.reshape(n_seq, seq, dim), d_table, d_attn_norm, d_query, d_key, d_value, d_q_norm, d_k_norm, d_out, d_mlp_norm, d_gate, d_up, d_down)

    return jax.shard_map(device_step, mesh=mesh, in_specs=(row_spec, row_spec, row_spec) + weight_specs + (batch_spec,), out_specs=(batch_spec, row_spec) + weight_specs, check_vma=False)
```
